32 devices in a mesh: section: 4 (over y, core), wide: 2 (over x), narrow: 4 (over z).
Axes of the slice: x: 2, y: 2, z: 4, core: 2. Of those that a mesh axis runs over, the one named last changes fastest.
Arguments:
- normed_inputs: bfloat16 [4, 4, 4, 192, 4096], P('section', 'narrow', None, 'wide'), may hold values from -160 to 160
- value_cotangent: bfloat16 [4, 4, 4, 192, 1024], P('section', 'narrow', None, 'wide'), may hold values from -6 to 6
- expert_hidden: bfloat16 [4, 4, 4, 64, 7168], P('section', 'narrow', None, None, 'wide'), may hold values from -40 to 40
- expert_cotangent: bfloat16 [4, 4, 4, 64, 4096], P('section', 'narrow', None, 'wide'), may hold values from -110 to 110
- slot_gate: bfloat16 [4, 4, 4, 64], P('section', 'narrow', None, 'wide'), may hold values from 0.25 to 1
- slot_count: int32 [4, 4, 4], P('section', 'narrow'), may hold values from 33 to 64, as said below
- expert_weight: bfloat16 [4, 7168, 4096], P('section', 'wide', 'narrow'), may hold values from -0.0625 to 0.0625
- expert_moment: float32 [4, 7168, 4096], P('section', 'wide', 'narrow'), may hold values from -6 to 6
- value_weight: bfloat16 [4, 4096, 1024], P('section', ('wide', 'narrow')), may hold values from -0.09375 to 0.09375
- value_moment: float32 [4, 4096, 1024], P('section', ('wide', 'narrow')), may hold values from -6 to 6
Outputs:
- expert_weight_next: bfloat16 [4, 7168, 4096], P('section', 'wide', 'narrow')
- expert_moment_next: float32 [4, 7168, 4096], P('section', 'wide', 'narrow')
- value_weight_next: bfloat16 [4, 4096, 1024], P('section', ('wide', 'narrow'))
- value_moment_next: float32 [4, 4096, 1024], P('section', ('wide', 'narrow'))
The draws below stay inside these ranges and needn't reach their ends.
Inputs may be any that keep to these rules, and one draw needn't show every extreme that they name: The live slots of a micro-batch are slots 0 to slot_count - 1; in every layer and replica some micro-batch fills all 64 slots.
All inputs are finite; a program needn't handle non-finite values.
Results may differ from the reference program's by a relative error of at most 0.014.
Values may be sent and summed in bfloat16 or wider, within the bound.
A program may use at most 192 MiB of HBM per device.

```python
import math
import jax
import jax.numpy as jnp
from jax import lax

D = 4096
FF = 7168
KV = 1024
MICRO = 4
MB_DEV = 96
SECTIONS = 4
REPLICAS = 4
SEQ = 192
SLOTS = 64
N_WIDE = 2


def rough_field(base_key, extent, section_rise, divisor):
    subkeys = jax.random.split(base_key, 3)
    columns = extent[-1]
    layers = extent[0]
    column_pos = jnp.arange(columns, dtype=jnp.float32) / max(columns - 1, 1)
    column_scale = jnp.exp(math.log(3.0) * column_pos + jax.random.uniform(subkeys[0], (columns,), jnp.float32, 0.0, math.log(3.3)))
    layer_pos = jnp.arange(layers, dtype=jnp.float32) / max(layers - 1, 1)
    layer_scale = jnp.exp(section_rise * math.log(3.0) * layer_pos).reshape(layers, 1, 1, 1, 1)
    row_scale = jnp.exp(jax.random.uniform(subkeys[1], extent[:-1] + (1,), jnp.float32, 0.0, math.log(3.0)))
    values = jnp.clip(jax.random.normal(subkeys[2], extent, jnp.float32), -6.0, 6.0)
    return values * row_scale * column_scale * layer_scale / divisor


def draw_normed_inputs(key, part):
    return rough_field(jax.random.fold_in(key, 3), (SECTIONS, REPLICAS, MICRO, SEQ, D), 1.0, 4.0).astype(jnp.bfloat16)


def draw_expert_hidden(key, part):
    return rough_field(jax.random.fold_in(key, 5), (SECTIONS, REPLICAS, MICRO, SLOTS, FF), 0.0, 6.0).astype(jnp.bfloat16)


def draw_expert_cotangent(key, part):
    return rough_field(jax.random.fold_in(key, 7), (SECTIONS, REPLICAS, MICRO, SLOTS, D), 1.0, 6.0).astype(jnp.bfloat16)


def draw_slot_count(key, part):
    count_key = jax.random.fold_in(key, 11)
    pick_key = jax.random.fold_in(key, 13)
    counts = jax.random.randint(count_key, (SECTIONS, REPLICAS, MICRO), SLOTS // 2 + 1, SLOTS + 1, dtype=jnp.int32)
    chosen = jax.random.randint(pick_key, (SECTIONS, REPLICAS, 1), 0, MICRO, dtype=jnp.int32)
    positions = jnp.arange(MICRO, dtype=jnp.int32).reshape(1, 1, MICRO)
    return jnp.where(positions == chosen, jnp.int32(SLOTS), counts).astype(jnp.int32)


def block_scale(key, dims, cuts, smallest, high):
    level = 1.0
    for position, parts in cuts:
        heights = jax.random.uniform(jax.random.fold_in(jax.random.fold_in(key, 6), position), (parts,), jnp.float32, smallest / len(cuts), high / len(cuts))
        level = level * jnp.repeat(jnp.exp(heights), dims[position] // parts).reshape((-1,) + (1,) * (len(dims) - 1 - position))
    return level


def scatter_about(key, shape, deviation, reach, shards=(), held_as=jnp.bfloat16):
    level = block_scale(key, shape, shards, -0.22, 0.18) if shards else 1.0
    entries = jax.random.normal(key, shape, jnp.float32) * deviation * level
    return jnp.minimum(jnp.maximum(entries, -reach), reach).astype(held_as)


def setup_inputs(seed: int = 0) -> dict:
    key_of = jax.random.split(jax.random.key(seed), 11)
    normed_inputs = draw_normed_inputs(jax.random.fold_in(key_of[10], 71), 0)
    value_cotangent = scatter_about(key_of[1], (SECTIONS, REPLICAS, MICRO, SEQ, KV), 1.0, 6.0, ((0, 4), (1, 4), (3, 2)))
    expert_hidden = draw_expert_hidden(jax.random.fold_in(key_of[10], 71), 0)
    expert_cotangent = draw_expert_cotangent(jax.random.fold_in(key_of[10], 71), 0)
    slot_gate = jnp.clip(0.25 + 0.75 * jax.random.uniform(key_of[4], (SECTIONS, REPLICAS, MICRO, SLOTS), jnp.float32) ** block_scale(key_of[4], (SECTIONS, REPLICAS, MICRO, SLOTS), ((0, 4), (1, 4), (3, 2)), -0.2, 0.2), 0.25, 1.0).astype(jnp.bfloat16)
    slot_count = draw_slot_count(jax.random.fold_in(key_of[10], 71), 0)
    expert_weight = scatter_about(key_of[6], (SECTIONS, FF, D), FF ** -0.5, 0.0625, ((0, 4), (1, 2), (2, 4)))
    expert_moment = scatter_about(key_of[7], (SECTIONS, FF, D), 1.0, 6.0, ((0, 4), (1, 2), (2, 4)), jnp.float32)
    value_weight = scatter_about(key_of[8], (SECTIONS, D, KV), D ** -0.5, 0.09375, ((0, 4), (1, 8)))
    value_moment = scatter_about(key_of[9], (SECTIONS, D, KV), 1.0, 6.0, ((0, 4), (1, 8)), jnp.float32)
    return {"normed_inputs": normed_inputs, "value_cotangent": value_cotangent, "expert_hidden": expert_hidden, "expert_cotangent": expert_cotangent, "slot_gate": slot_gate, "slot_count": slot_count, "expert_weight": expert_weight, "expert_moment": expert_moment, "value_weight": value_weight, "value_moment": value_moment}


MOMENTUM_DECAY = 0.9
STEP_RATE = 0.01

def rounded_add(accumulated, product):
    kept = lax.optimization_barrier(product.astype(jnp.bfloat16))
    return accumulated + kept.astype(jnp.float32)

def expert_layer(hidden_layer, cotangent_layer, gate_layer, count_layer):
    positions = jnp.arange(SLOTS, dtype=jnp.int32)
    live = positions[None, None, :] < count_layer[:, :, None]
    coefficient = jnp.where(live, gate_layer.astype(jnp.float32), jnp.zeros(gate_layer.shape, jnp.float32))
    scaled = (coefficient[..., None] * cotangent_layer.astype(jnp.float32)).astype(jnp.bfloat16)

    def add_replica(accumulated, pieces):
        hidden_rows = pieces[0].reshape(-1, FF)
        scaled_rows = pieces[1].reshape(-1, D)
        product = jnp.dot(hidden_rows.T, scaled_rows, preferred_element_type=jnp.float32)
        return (rounded_add(accumulated, product), None)
    result, ignored = lax.scan(add_replica, jnp.zeros((FF, D), jnp.float32), (hidden_layer, scaled))
    return result

def value_layer(input_layer, cotangent_layer):
    device_inputs = input_layer.reshape(REPLICAS, MICRO, N_WIDE, MB_DEV, D).transpose(0, 2, 1, 3, 4).reshape(REPLICAS * N_WIDE, MICRO * MB_DEV, D)
    device_cotangents = cotangent_layer.reshape(REPLICAS, MICRO, N_WIDE, MB_DEV, KV).transpose(0, 2, 1, 3, 4).reshape(REPLICAS * N_WIDE, MICRO * MB_DEV, KV)

    def add_device(accumulated, pieces):
        product = jnp.dot(pieces[0].T, pieces[1], preferred_element_type=jnp.float32)
        return (rounded_add(accumulated, product), None)
    result, ignored = lax.scan(add_device, jnp.zeros((D, KV), jnp.float32), (device_inputs, device_cotangents))
    return result

def reference(normed_inputs, value_cotangent, expert_hidden, expert_cotangent, slot_gate, slot_count, expert_weight, expert_moment, value_weight, value_moment):
    expert_grads = []
    value_grads = []
    for layer_index in range(SECTIONS):
        expert_grads.append(expert_layer(expert_hidden[layer_index], expert_cotangent[layer_index], slot_gate[layer_index], slot_count[layer_index]))
        value_grads.append(value_layer(normed_inputs[layer_index], value_cotangent[layer_index]))
    expert_grad = jnp.stack(expert_grads)
    value_grad = jnp.stack(value_grads)
    overall = jnp.sum(expert_grad * expert_grad) + jnp.sum(value_grad * value_grad)
    entry_count = SECTIONS * (FF * D + D * KV)
    factor = jnp.minimum(1.0, math.sqrt(entry_count) / jnp.sqrt(overall + 1e-06))
    expert_next = MOMENTUM_DECAY * expert_moment + factor * expert_grad
    value_next = MOMENTUM_DECAY * value_moment + factor * value_grad
    expert_weight_next = (expert_weight.astype(jnp.float32) - STEP_RATE * expert_next).astype(jnp.bfloat16)
    value_weight_next = (value_weight.astype(jnp.float32) - STEP_RATE * value_next).astype(jnp.bfloat16)
    return (expert_weight_next, expert_next, value_weight_next, value_next)
```

```python
import functools
import math

import jax
import jax.numpy as jnp
from jax import lax
from jax.experimental import pallas as pl
from jax.experimental.pallas import tpu as pltpu
from jax.sharding import PartitionSpec as P

MOMENTUM_DECAY = 0.9
STEP_RATE = 0.01
MESH = pl.DeviceIdType.MESH
F32 = jnp.float32
BF16 = jnp.bfloat16
RS_PIECES = 2


def column_chunks(width):
    lanes = width // 128
    return max(c for c in range(1, 9) if lanes % c == 0)


def grant(scratch, *arrays):
    held = [(math.prod(a.shape), a.dtype) for a in arrays]
    held += [(math.prod(a.inner_aval.shape), a.inner_aval.dtype) for a in scratch]
    return sum(n * d.itemsize for n, d in held) + 2 * 2**20


def dot_rows(a, b):
    return lax.dot_general(a, b, (((0,), (0,)), ((), ())), preferred_element_type=F32)


def gather_kernel(
    dims,
    x_ref,
    vc_ref,
    h_ref,
    cot_ref,
    coef_ref,
    mom_ref,
    *refs,
):
    n_section, n_wide, n_narrow, chunks = dims
    egrads, emoms, refs = refs[:chunks], refs[chunks : 2 * chunks], refs[2 * chunks :]
    run_gather(dims, x_ref, vc_ref, h_ref, cot_ref, coef_ref, mom_ref, egrads, emoms, *refs)


def run_gather(
    dims,
    x_ref,
    vc_ref,
    h_ref,
    cot_ref,
    coef_ref,
    mom_ref,
    egrads,
    emoms,
    vgrad,
    total,
    hbuf,
    sbuf,
    scaled,
    rows,
    cots,
    part,
    rbuf,
    rlast,
    sums,
    mine,
    h_recv,
    h_right,
    h_left,
    s_recv,
    s_send,
    s_relay,
    x_recv,
    x_send,
    r_recv,
    r_last,
    r_right,
    r_left,
    g_recv,
    g_send,
    local,
):
    n_section, n_wide, n_narrow, chunks = dims
    si, wi, ni = lax.axis_index("section"), lax.axis_index("wide"), lax.axis_index("narrow")
    last = n_narrow - 1
    tokens = x_ref.shape[0]
    h_rows = h_ref.shape[0]
    c_width = h_ref.shape[1] // chunks
    r_width = rows.shape[2]
    s_width = sbuf.shape[4]
    piece = r_width // RS_PIECES
    dest_order = [d for pair in zip(range(last, -1, -1), range(n_narrow)) for d in pair]
    dest_order = list(dict.fromkeys(dest_order))

    def at(section=0, wide=0, narrow=0):
        return (
            lax.rem(si + section, n_section),
            lax.rem(wi + wide, n_wide),
            lax.rem(ni + narrow, n_narrow),
        )

    def remote(src, dst, send_sem, recv_sem, device):
        return pltpu.make_async_remote_copy(
            src_ref=src,
            dst_ref=dst,
            send_sem=send_sem,
            recv_sem=recv_sem,
            device_id=device,
            device_id_type=MESH,
        )

    right, left = (si, wi, jnp.minimum(ni + 1, last)), (si, wi, jnp.maximum(ni - 1, 0))
    groups = [
        [(0, w, n) for w in range(n_wide) for n in range(n_narrow) if w or n],
        [(s, 0, 0) for s in range(1, n_section)],
    ]

    own = []
    own.append(
        pltpu.make_async_copy(vc_ref, cots.at[pl.ds(wi * tokens, tokens)], local.at[0])
    )
    for d in range(n_narrow):
        start = pl.multiple_of((wi * n_narrow + d) * r_width, r_width)
        own.append(
            pltpu.make_async_copy(
                x_ref.at[:, pl.ds(start, r_width)],
                rows.at[d, pl.ds(wi * tokens, tokens)],
                local.at[1 + d],
            )
        )
    own_hidden = [
        pltpu.make_async_copy(
            h_ref.at[:, pl.ds(c * c_width, c_width)],
            hbuf.at[c, pl.ds(ni * h_rows, h_rows)],
            local.at[1 + n_narrow + c],
        )
        for c in range(chunks)
    ]
    own_moment = [
        pltpu.make_async_copy(
            mom_ref.at[pl.ds(c * c_width, c_width)],
            emoms[c],
            local.at[1 + n_narrow + chunks + c],
        )
        for c in range(chunks)
    ]
    for copy in own + own_hidden:
        copy.start()

    barrier = pltpu.get_barrier_semaphore()
    n_peers = 0
    for group in groups:
        for offset in group:
            pl.semaphore_signal(barrier, inc=1, device_id=at(*offset), device_id_type=MESH)
            n_peers += 1
    pl.semaphore_wait(barrier, n_peers)

    def hidden_copy(r, c, rightward, first):
        block = hbuf.at[c, pl.ds(r * h_rows, h_rows)]
        src = h_ref.at[:, pl.ds(c * c_width, c_width)] if first else block
        sems = h_right if rightward else h_left
        return remote(src, block, sems.at[r, c], h_recv.at[r, c], right if rightward else left)

    def send_own_hidden(c):
        @pl.when(ni < last)
        def _():
            hidden_copy(ni, c, True, True).start()

        @pl.when(ni > 0)
        def _():
            hidden_copy(ni, c, False, True).start()

    def hidden_step(k, c):
        @pl.when(ni >= k)
        def _():
            hidden_copy(ni - k, c, True, False).wait_recv()

            @pl.when(ni < last)
            def _():
                hidden_copy(ni - k, c, True, False).start()

        @pl.when(ni + k <= last)
        def _():
            hidden_copy(ni + k, c, False, False).wait_recv()

            @pl.when(ni > 0)
            def _():
                hidden_copy(ni + k, c, False, False).start()

    def wide_vc(k, source):
        return remote(
            vc_ref,
            cots.at[pl.ds(source * tokens, tokens)],
            x_send.at[k, n_narrow],
            x_recv.at[source, n_narrow],
            at(0, k, 0),
        )

    def wide_rows(k, d, source):
        peer = lax.rem(wi + k, n_wide)
        start = pl.multiple_of((peer * n_narrow + d) * r_width, r_width)
        return remote(
            x_ref.at[:, pl.ds(start, r_width)],
            rows.at[d, pl.ds(source * tokens, tokens)],
            x_send.at[k, d],
            x_recv.at[source, d],
            at(0, k, 0),
        )

    def slot_copy(k):
        peer = lax.rem(ni + k, n_narrow)
        start = pl.multiple_of(peer * s_width, s_width)
        return remote(
            scaled.at[:, :, pl.ds(start, s_width)],
            sbuf.at[ni, :, wi],
            s_send.at[k],
            s_recv.at[ni, wi],
            at(0, 0, k),
        )

    def slot_relay(r, k):
        return remote(
            sbuf.at[r, :, wi],
            sbuf.at[r, :, wi],
            s_relay.at[r, k],
            s_recv.at[r, wi],
            at(0, k, 0),
        )

    def slot_arrival(r, w):
        return remote(sbuf.at[r, :, w], sbuf.at[r, :, w], s_send.at[0], s_recv.at[r, w], right)

    for k in range(1, n_wide):
        wide_vc(k, wi).start()
    for d in dest_order:
        for k in range(1, n_wide):
            wide_rows(k, d, wi).start()
    for c in range(0, 2):
        send_own_hidden(c)

    scaled[...] = (coef_ref[:, :, 0:1] * cot_ref[...].astype(F32)).astype(BF16)
    for k in range(1, n_narrow):
        slot_copy(k).start()
    for c in range(2, chunks):
        send_own_hidden(c)
    for copy in own_moment:
        copy.start()
    own_start = pl.multiple_of(ni * s_width, s_width)
    sbuf[ni, :, wi] = scaled[:, :, pl.ds(own_start, s_width)]
    for k in range(1, n_wide):
        slot_relay(ni, k).start()

    def make_part(d):
        if d == dest_order[0]:
            own[0].wait()
            for k in range(1, n_wide):
                wide_vc(k, lax.rem(wi + n_wide - k, n_wide)).wait_recv()
        own[1 + d].wait()
        for k in range(1, n_wide):
            wide_rows(k, d, lax.rem(wi + n_wide - k, n_wide)).wait_recv()
        part[d] = dot_rows(rows[d], cots[...]).astype(BF16)

    def piece_at(ref, d, q):
        return ref.at[d, pl.ds(q * piece, piece)]

    def sum_copy(d, q, rightward, final):
        dst = rlast.at[pl.ds(q * piece, piece)] if final else piece_at(rbuf, d, q)
        sem = r_last.at[q] if final else r_recv.at[d, q]
        sems = r_right if rightward else r_left
        return remote(piece_at(part, d, q), dst, sems.at[d, q], sem, right if rightward else left)

    def sum_send(i, d, rightward):
        final_right = rightward and d == i + 1
        for q in range(RS_PIECES):
            sum_copy(d, q, rightward, final_right).start()

    def sum_slot(slot):
        for i in range(1, n_narrow):
            j = slot - 2 * (i - 1)
            if j < 0 or j > last - i:
                continue
            for rightward in (True, False):
                me = i if rightward else last - i
                d = last - j if rightward else j

                @pl.when(ni == me)
                def _(me=me, d=d, rightward=rightward):
                    final = d == me
                    landing = final and rightward
                    for q in range(RS_PIECES):
                        sum_copy(d, q, rightward, landing).wait_recv()
                        rs = pl.ds(q * piece, piece)
                        came = rlast[rs] if landing else rbuf[d, rs]
                        if final:
                            vgrad[rs] += came.astype(F32)
                        else:
                            part[d, rs] = (part[d, rs].astype(F32) + came.astype(F32)).astype(BF16)
                            ahead = me + 1 if rightward else me - 1
                            sum_copy(d, q, rightward, rightward and d == ahead).start()

    def originate(d):
        if d > 0:

            @pl.when(ni == 0)
            def _():
                sum_send(0, d, True)

        if d < last:

            @pl.when(ni == last)
            def _():
                sum_send(last, d, False)

    mine[...] = jnp.zeros_like(mine)

    def add_squares(block):
        sq = block * block
        n_rows, n_cols = sq.shape
        folded = jnp.sum(sq.reshape(n_rows // 8, 8, n_cols), axis=0)
        acc = folded[:, 0:128]
        for lane in range(128, n_cols, 128):
            acc = acc + folded[:, lane : lane + 128]
        mine[...] += acc

    right_side = sbuf.at[...]

    def expert_chunk(c):
        product = dot_rows(hbuf[c], right_side[...].reshape(-1, s_width))
        egrads[c][...] = product
        add_squares(product)

    todo = list(dest_order)
    for k in range(1, n_narrow):
        for c in range(chunks):
            hidden_step(k, c)
            if k == 1 and c >= 3 and (c - 3) % 2 == 0 and len(todo) > 2:
                d = todo.pop(0)
                make_part(d)
                originate(d)
            if k == 2 and c == 1:
                while todo:
                    make_part(todo.pop(0))
                for d in dest_order[2:]:
                    if d > 0:

                        @pl.when(ni == 0)
                        def _(d=d):
                            sum_send(0, d, True)

                for d in dest_order[:1:-1]:
                    if d < last:

                        @pl.when(ni == last)
                        def _(d=d):
                            sum_send(last, d, False)

                vgrad[...] = part[ni].astype(F32)
            if k == 2 and c == 3:
                for j in range(1, n_narrow):
                    r = lax.rem(ni + n_narrow - j, n_narrow)
                    slot_arrival(r, wi).wait_recv()
                    for m in range(1, n_wide):
                        slot_relay(r, m).start()
            if k == 2 and c == chunks - 1:
                sum_slot(0)
                for copy in own_hidden:
                    copy.wait()
                for j in range(n_narrow):
                    for m in range(1, n_wide):
                        slot_arrival(j, lax.rem(wi + m, n_wide)).wait_recv()
            if k == 3:
                expert_chunk(c)
                if c % 2 == 1:
                    sum_slot(1 + c // 2)
    sum_slot(4)
    add_squares(vgrad[...])

    index = 0
    for group in groups:
        base = index
        for offset in group:
            remote(mine, sums.at[index], g_send.at[index], g_recv.at[index], at(*offset)).start()
            index += 1
        for i in range(base, index):
            remote(mine, sums.at[i], g_send.at[i], g_recv.at[i], right).wait_send()
        for i in range(base, index):
            remote(mine, sums.at[i], g_send.at[i], g_recv.at[i], right).wait_recv()
        mine[...] = mine[...] + jnp.sum(sums[base:index], axis=0)
    overall = jnp.sum(mine[...])
    total[...] = jnp.zeros_like(total) + overall

    for copy in own_moment:
        copy.wait()
    for c in range(chunks):
        for k in range(n_narrow):

            @pl.when((ni >= k) & (ni < last))
            def _(k=k, c=c):
                hidden_copy(ni - k, c, True, False).wait_send()

            @pl.when((ni + k <= last) & (ni > 0))
            def _(k=k, c=c):
                hidden_copy(ni + k, c, False, False).wait_send()

    for k in range(1, n_wide):
        wide_vc(k, wi).wait_send()
        for d in range(n_narrow):
            wide_rows(k, d, wi).wait_send()
        for r in range(n_narrow):
            slot_relay(r, k).wait_send()
    for k in range(1, n_narrow):
        slot_copy(k).wait_send()
    for d in range(n_narrow):
        for q in range(RS_PIECES):

            @pl.when(ni < d)
            def _(d=d, q=q):
                sum_copy(d, q, True, False).wait_send()

            @pl.when(ni > d)
            def _(d=d, q=q):
                sum_copy(d, q, False, False).wait_send()


def update_kernel(entries, chunks, split, slots, total, vgrad, *refs):
    run_update(entries, split, slots, total, vgrad, refs[:chunks], refs[chunks : 2 * chunks], *refs[2 * chunks :])


def run_update(
    entries,
    split,
    slots,
    total,
    vgrad,
    egrads,
    emoms,
    ew_ref,
    vm_ref,
    vw_ref,
    ew_out,
    em_out,
    vw_out,
    vm_out,
    weights,
    vmom,
    vweights,
    em_stage,
    ew_stage,
    vm_stage,
    vw_stage,
    in_sem,
    out_sem,
    v_sem,
):
    tile = egrads[0].shape[0] // split
    tiles = len(egrads) * split

    def weight_in(t):
        rs = pl.ds(t * tile, tile)
        return pltpu.make_async_copy(ew_ref.at[rs], weights.at[rs], in_sem.at[t])

    def out(t):
        rs = pl.ds(t * tile, tile)
        slot = t % slots
        return (
            pltpu.make_async_copy(em_stage.at[slot], em_out.at[rs], out_sem.at[slot, 0]),
            pltpu.make_async_copy(ew_stage.at[slot], ew_out.at[rs], out_sem.at[slot, 1]),
        )

    for t in range(tiles):
        weight_in(t).start()
    v_in = (
        pltpu.make_async_copy(vm_ref, vmom, v_sem.at[0]),
        pltpu.make_async_copy(vw_ref, vweights, v_sem.at[1]),
    )
    v_out = (
        pltpu.make_async_copy(vm_stage, vm_out, v_sem.at[2]),
        pltpu.make_async_copy(vw_stage, vw_out, v_sem.at[3]),
    )
    for copy in v_in:
        copy.start()
    factor = jnp.minimum(1.0, math.sqrt(entries) / jnp.sqrt(total[0:1, 0:1] + 1e-06))
    for t in range(tiles):
        rs = pl.ds(t * tile, tile)
        slot = t % slots
        if t >= slots:
            for copy in out(t - slots):
                copy.wait()
        weight_in(t).wait()
        inner = pl.ds(t % split * tile, tile)
        moment = MOMENTUM_DECAY * emoms[t // split][inner] + factor * egrads[t // split][inner]
        em_stage[slot] = moment
        ew_stage[slot] = (weights[rs].astype(F32) - STEP_RATE * moment).astype(BF16)
        for copy in out(t):
            copy.start()
    for copy in v_in:
        copy.wait()
    moment = MOMENTUM_DECAY * vmom[...] + factor * vgrad[...]
    vm_stage[...] = moment
    vw_stage[...] = (vweights[...].astype(F32) - STEP_RATE * moment).astype(BF16)
    for copy in v_out:
        copy.start()
    for t in range(max(tiles - slots, 0), tiles):
        for copy in out(t):
            copy.wait()
    for copy in v_out:
        copy.wait()


def on_device(
    normed_inputs,
    value_cotangent,
    expert_hidden,
    expert_cotangent,
    slot_gate,
    slot_count,
    expert_weight,
    expert_moment,
    value_weight,
    value_moment,
):
    n_section = lax.axis_size("section")
    n_wide = lax.axis_size("wide")
    n_narrow = lax.axis_size("narrow")
    width, kv = normed_inputs.shape[-1], value_cotangent.shape[-1]
    x = normed_inputs.reshape(-1, width)
    vc = value_cotangent.reshape(-1, kv)
    hidden = expert_hidden.reshape(-1, expert_hidden.shape[-1])
    cotangent = expert_cotangent[0, 0]
    micro, slots, _ = cotangent.shape
    positions = lax.axis_index("wide") * slots + jnp.arange(slots, dtype=jnp.int32)
    live = positions[None, :] < slot_count[0, 0][:, None]
    coefficient = jnp.where(live, slot_gate[0, 0].astype(F32), 0.0)
    coefficient = jnp.broadcast_to(coefficient[:, :, None], (micro, slots, 128))

    tokens = x.shape[0]
    h_rows, ff = hidden.shape
    chunks = column_chunks(ff)
    r_width = width // (n_wide * n_narrow)
    s_width = width // n_narrow
    piece = RS_PIECES
    peers = n_wide * n_narrow - 1 + n_section - 1
    dma = pltpu.SemaphoreType.DMA
    hbm = pl.BlockSpec(memory_space=pl.ANY)
    vmem = pl.BlockSpec(memory_space=pltpu.VMEM)
    block = pltpu.VMEM((ff // chunks, s_width), F32)
    scratch = [
        pltpu.VMEM((chunks, n_narrow * h_rows, ff // chunks), BF16),
        pltpu.VMEM((n_narrow, micro, n_wide, slots, s_width), BF16),
        pltpu.VMEM((micro, slots, width), BF16),
        pltpu.VMEM((n_narrow, n_wide * tokens, r_width), BF16),
        pltpu.VMEM((n_wide * tokens, kv), BF16),
        pltpu.VMEM((n_narrow, r_width, kv), BF16),
        pltpu.VMEM((n_narrow, r_width, kv), BF16),
        pltpu.VMEM((r_width, kv), BF16),
        pltpu.VMEM((peers, 8, 128), F32),
        pltpu.VMEM((8, 128), F32),
    ]
    *blocks, vgrad, total = pl.pallas_call(
        functools.partial(gather_kernel, (n_section, n_wide, n_narrow, chunks)),
        out_shape=(
            *[block] * (2 * chunks),
            pltpu.VMEM((r_width, kv), F32),
            pltpu.VMEM((8, 128), F32),
        ),
        in_specs=[hbm, hbm, hbm, vmem, vmem, hbm],
        out_specs=(vmem,) * (2 * chunks + 2),
        scratch_shapes=[
            *scratch,
            dma((n_narrow, chunks)),
            dma((n_narrow, chunks)),
            dma((n_narrow, chunks)),
            dma((n_narrow, n_wide)),
            dma((n_narrow,)),
            dma((n_narrow, n_wide)),
            dma((n_wide, n_narrow + 1)),
            dma((n_wide, n_narrow + 1)),
            dma((n_narrow, piece)),
            dma((piece,)),
            dma((n_narrow, piece)),
            dma((n_narrow, piece)),
            dma((peers,)),
            dma((peers,)),
            dma((1 + n_narrow + 2 * chunks,)),
        ],
        compiler_params=pltpu.CompilerParams(
            collective_id=0, has_side_effects=True, vmem_limit_bytes=grant(scratch, cotangent, coefficient)
        ),
    )(x, vc, hidden, cotangent, coefficient, expert_moment[0])

    total, vgrad, *blocks = (
        pltpu.with_memory_space_constraint(a, pltpu.VMEM) for a in (total, vgrad, *blocks)
    )
    layer_entries = ff * s_width + r_width * kv
    entries = n_section * n_wide * n_narrow * layer_entries
    split, depth = 2, 4
    tiles = chunks * split
    tile = ff // tiles
    update_scratch = [
        pltpu.VMEM((ff, s_width), BF16),
        pltpu.VMEM((r_width, kv), F32),
        pltpu.VMEM((r_width, kv), BF16),
        pltpu.VMEM((depth, tile, s_width), F32),
        pltpu.VMEM((depth, tile, s_width), BF16),
        pltpu.VMEM((r_width, kv), F32),
        pltpu.VMEM((r_width, kv), BF16),
    ]
    outs = pl.pallas_call(
        functools.partial(update_kernel, entries, chunks, split, depth),
        out_shape=(
            jax.ShapeDtypeStruct((ff, s_width), BF16),
            jax.ShapeDtypeStruct((ff, s_width), F32),
            jax.ShapeDtypeStruct((r_width, kv), BF16),
            jax.ShapeDtypeStruct((r_width, kv), F32),
        ),
        in_specs=[vmem] * (2 * chunks + 2) + [hbm] * 3,
        out_specs=(hbm, hbm, hbm, hbm),
        scratch_shapes=[
            *update_scratch,
            dma((tiles,)),
            dma((depth, 2)),
            dma((4,)),
        ],
        compiler_params=pltpu.CompilerParams(vmem_limit_bytes=grant(update_scratch)),
    )(total, vgrad, *blocks, expert_weight[0], value_moment[0], value_weight[0])
    return tuple(o[None] for o in outs)


def solution(mesh):
    return jax.shard_map(
        on_device,
        mesh=mesh,
        in_specs=(
            P("section", "narrow", None, "wide", None),
            P("section", "narrow", None, "wide", None),
            P("section", "narrow", None, None, "wide"),
            P("section", "narrow", None, "wide", None),
            P("section", "narrow", None, "wide"),
            P("section", "narrow", None),
            P("section", "wide", "narrow"),
            P("section", "wide", "narrow"),
            P("section", ("wide", "narrow"), None),
            P("section", ("wide", "narrow"), None),
        ),
        out_specs=(
            P("section", "wide", "narrow"),
            P("section", "wide", "narrow"),
            P("section", ("wide", "narrow"), None),
            P("section", ("wide", "narrow"), None),
        ),
        check_vma=False,
    )
```

```python
import functools
import math

import jax
import jax.numpy as jnp
from jax import lax
from jax.experimental import pallas as pl
from jax.experimental.pallas import tpu as pltpu
from jax.sharding import PartitionSpec as P

MOMENTUM_DECAY = 0.9
STEP_RATE = 0.01
MESH = pl.DeviceIdType.MESH
F32 = jnp.float32
BF16 = jnp.bfloat16
RS_PIECES = 2


def column_chunks(width):
    lanes = width // 128
    return max(c for c in range(1, 9) if lanes % c == 0)


def grant(scratch, *arrays):
    held = [(math.prod(a.shape), a.dtype) for a in arrays]
    held += [(math.prod(a.inner_aval.shape), a.inner_aval.dtype) for a in scratch]
    return sum(n * d.itemsize for n, d in held) + 4 * 2**20


def dot_rows(a, b):
    return lax.dot_general(a, b, (((0,), (0,)), ((), ())), preferred_element_type=F32)


def gather_kernel(
    dims,
    x_ref,
    vc_ref,
    h_ref,
    cot_ref,
    gate_ref,
    count_ref,
    mom_ref,
    w_ref,
    *refs,
):
    n_section, n_wide, n_narrow, chunks = dims
    arrays = (x_ref, vc_ref, h_ref, cot_ref, gate_ref, count_ref, mom_ref, w_ref)
    egrads, emoms, refs = refs[:chunks], refs[chunks : 2 * chunks], refs[2 * chunks :]
    run_gather(dims, *arrays, egrads, emoms, refs[:chunks], *refs[chunks:])


def run_gather(
    dims,
    x_ref,
    vc_ref,
    h_ref,
    cot_ref,
    gate_ref,
    count_ref,
    mom_ref,
    w_ref,
    egrads,
    emoms,
    hbuf,
    vgrad,
    total,
    sbuf,
    scaled,
    rows,
    cots,
    part,
    rbuf,
    rlast,
    sums,
    own_sum,
    mine,
    h_recv,
    h_right,
    h_left,
    s_recv,
    s_send,
    s_relay,
    x_recv,
    x_send,
    r_recv,
    r_last,
    r_right,
    r_left,
    g_recv,
    g_send,
    local,
):
    n_section, n_wide, n_narrow, chunks = dims
    si, wi, ni = lax.axis_index("section"), lax.axis_index("wide"), lax.axis_index("narrow")
    last = n_narrow - 1
    tokens = x_ref.shape[0]
    h_rows = h_ref.shape[0]
    c_width = h_ref.shape[1] // chunks
    r_width = rows.shape[2]
    s_width = sbuf.shape[4]
    piece = r_width // RS_PIECES
    dest_order = [d for pair in zip(range(last, -1, -1), range(n_narrow)) for d in pair]
    dest_order = list(dict.fromkeys(dest_order))

    def at(section=0, wide=0, narrow=0):
        return (
            lax.rem(si + section, n_section),
            lax.rem(wi + wide, n_wide),
            lax.rem(ni + narrow, n_narrow),
        )

    def remote(src, dst, send_sem, recv_sem, device):
        return pltpu.make_async_remote_copy(
            src_ref=src,
            dst_ref=dst,
            send_sem=send_sem,
            recv_sem=recv_sem,
            device_id=device,
            device_id_type=MESH,
        )

    right, left = (si, wi, jnp.minimum(ni + 1, last)), (si, wi, jnp.maximum(ni - 1, 0))
    n_devices = n_section * n_wide * n_narrow
    greeted = [(s, 0, 0) for s in range(1, n_section)]
    greeted += [(0, w, 0) for w in range(1, n_wide)]
    greeted += [(0, 0, n) for n in range(1, n_narrow)]

    barrier = pltpu.get_barrier_semaphore()
    for offset in greeted:
        pl.semaphore_signal(barrier, inc=1, device_id=at(*offset), device_id_type=MESH)

    own = []
    own.append(
        pltpu.make_async_copy(vc_ref, cots.at[pl.ds(wi * tokens, tokens)], local.at[0])
    )
    for d in range(n_narrow):
        start = pl.multiple_of((wi * n_narrow + d) * r_width, r_width)
        own.append(
            pltpu.make_async_copy(
                x_ref.at[:, pl.ds(start, r_width)],
                rows.at[d, pl.ds(wi * tokens, tokens)],
                local.at[1 + d],
            )
        )
    own_hidden = [
        pltpu.make_async_copy(
            h_ref.at[:, pl.ds(c * c_width, c_width)],
            hbuf[c].at[pl.ds(ni * h_rows, h_rows)],
            local.at[1 + n_narrow + c],
        )
        for c in range(chunks)
    ]
    own_moment = [
        pltpu.make_async_copy(
            mom_ref.at[pl.ds(c * c_width, c_width)],
            emoms[c],
            local.at[1 + n_narrow + chunks + c],
        )
        for c in range(chunks)
    ]
    own_slots = pltpu.make_async_copy(cot_ref, scaled, local.at[1 + n_narrow + 2 * chunks])
    blocks = s_width // c_width
    own_weights = [
        pltpu.make_async_copy(
            w_ref.at[pl.ds(c * c_width, c_width), pl.ds(j * c_width, c_width)],
            hbuf[c].at[pl.ds(j * c_width, c_width)],
            local.at[2 + n_narrow + 2 * chunks + c * blocks + j],
        )
        for c in range(chunks)
        for j in range(blocks)
    ]
    for copy in [own_slots] + own + own_hidden:
        copy.start()

    pl.semaphore_wait(barrier, len(greeted))

    def hidden_copy(r, c, rightward, first):
        block = hbuf[c].at[pl.ds(r * h_rows, h_rows)]
        src = h_ref.at[:, pl.ds(c * c_width, c_width)] if first else block
        sems = h_right if rightward else h_left
        return remote(src, block, sems.at[r, c], h_recv.at[r, c], right if rightward else left)

    def send_own_hidden(c):
        @pl.when(ni < last)
        def _():
            hidden_copy(ni, c, True, True).start()

        @pl.when(ni > 0)
        def _():
            hidden_copy(ni, c, False, True).start()

    def hidden_step(k, c):
        @pl.when(ni >= k)
        def _():
            hidden_copy(ni - k, c, True, False).wait_recv()

            @pl.when(ni < last)
            def _():
                hidden_copy(ni - k, c, True, False).start()

        @pl.when(ni + k <= last)
        def _():
            hidden_copy(ni + k, c, False, False).wait_recv()

            @pl.when(ni > 0)
            def _():
                hidden_copy(ni + k, c, False, False).start()

    def wide_vc(k, source):
        return remote(
            vc_ref,
            cots.at[pl.ds(source * tokens, tokens)],
            x_send.at[k, n_narrow],
            x_recv.at[source, n_narrow],
            at(0, k, 0),
        )

    def wide_rows(k, d, source):
        peer = lax.rem(wi + k, n_wide)
        start = pl.multiple_of((peer * n_narrow + d) * r_width, r_width)
        return remote(
            x_ref.at[:, pl.ds(start, r_width)],
            rows.at[d, pl.ds(source * tokens, tokens)],
            x_send.at[k, d],
            x_recv.at[source, d],
            at(0, k, 0),
        )

    def slot_copy(k):
        peer = lax.rem(ni + k, n_narrow)
        start = pl.multiple_of(peer * s_width, s_width)
        return remote(
            scaled.at[:, :, pl.ds(start, s_width)],
            sbuf.at[ni, :, wi],
            s_send.at[k],
            s_recv.at[ni, wi],
            at(0, 0, k),
        )

    def slot_relay(r, k):
        return remote(
            sbuf.at[r, :, wi],
            sbuf.at[r, :, wi],
            s_relay.at[r, k],
            s_recv.at[r, wi],
            at(0, k, 0),
        )

    def slot_arrival(r, w):
        return remote(sbuf.at[r, :, w], sbuf.at[r, :, w], s_send.at[0], s_recv.at[r, w], right)

    for c in range(0, 2):
        send_own_hidden(c)
    for k in range(1, n_wide):
        wide_vc(k, wi).start()
    for d in dest_order:
        for k in range(1, n_wide):
            wide_rows(k, d, wi).start()

    own_slots.wait()
    slots = scaled.shape[1]
    down = lax.broadcasted_iota(jnp.int32, (slots, slots), 0)
    across = lax.broadcasted_iota(jnp.int32, (slots, slots), 1)
    for m in range(scaled.shape[0]):
        live = wi * slots + across < count_ref[0:1, m : m + 1]
        gates = jnp.where(live & (down == across), gate_ref[m : m + 1, :].astype(F32), 0.0)
        coefficient = jnp.sum(gates, axis=1, keepdims=True)
        scaled[m] = (coefficient * scaled[m].astype(F32)).astype(BF16)
    for k in range(1, n_narrow):
        slot_copy(k).start()
    for c in range(2, chunks):
        send_own_hidden(c)
    for copy in own_moment:
        copy.start()
    own_start = pl.multiple_of(ni * s_width, s_width)
    sbuf[ni, :, wi] = scaled[:, :, pl.ds(own_start, s_width)]
    for k in range(1, n_wide):
        slot_relay(ni, k).start()

    def make_part(d):
        if d == dest_order[0]:
            own[0].wait()
            for k in range(1, n_wide):
                wide_vc(k, lax.rem(wi + n_wide - k, n_wide)).wait_recv()
        own[1 + d].wait()
        for k in range(1, n_wide):
            wide_rows(k, d, lax.rem(wi + n_wide - k, n_wide)).wait_recv()
        part[d] = dot_rows(rows[d], cots[...]).astype(BF16)

    mine[...] = jnp.zeros_like(mine)

    def add_squares(block):
        sq = block * block
        n_rows, n_cols = sq.shape
        folded = jnp.sum(sq.reshape(n_rows // 8, 8, n_cols), axis=0)
        acc = folded[:, 0:128]
        for lane in range(128, n_cols, 128):
            acc = acc + folded[:, lane : lane + 128]
        mine[...] += acc

    def piece_at(ref, d, q):
        return ref.at[d, pl.ds(q * piece, piece)]

    def sum_copy(d, q, rightward, final):
        dst = rlast.at[pl.ds(q * piece, piece)] if final else piece_at(rbuf, d, q)
        sem = r_last.at[q] if final else r_recv.at[d, q]
        sems = r_right if rightward else r_left
        return remote(piece_at(part, d, q), dst, sems.at[d, q], sem, right if rightward else left)

    def sum_send(i, d, rightward):
        final_right = rightward and d == i + 1
        for q in range(RS_PIECES):
            sum_copy(d, q, rightward, final_right).start()

    def sum_slot(slot):
        for i in range(1, n_narrow):
            j = slot - 2 * (i - 1)
            if j < 0 or j > last - i:
                continue
            for rightward in (True, False):
                me = i if rightward else last - i
                d = last - j if rightward else j

                @pl.when(ni == me)
                def _(me=me, d=d, rightward=rightward):
                    final = d == me
                    landing = final and rightward
                    for q in range(RS_PIECES):
                        sum_copy(d, q, rightward, landing).wait_recv()
                        rs = pl.ds(q * piece, piece)
                        came = rlast[rs] if landing else rbuf[d, rs]
                        if final:
                            done = vgrad[rs] + came.astype(F32)
                            vgrad[rs] = done
                            if me in (0, last) or rightward == (2 * me > last):
                                add_squares(done)
                        else:
                            part[d, rs] = (part[d, rs].astype(F32) + came.astype(F32)).astype(BF16)
                            ahead = me + 1 if rightward else me - 1
                            sum_copy(d, q, rightward, rightward and d == ahead).start()

    def originate(d):
        if d > 0:

            @pl.when(ni == 0)
            def _():
                sum_send(0, d, True)

        if d < last:

            @pl.when(ni == last)
            def _():
                sum_send(last, d, False)

    right_side = sbuf.at[...]

    def expert_chunk(c):
        product = dot_rows(hbuf[c][...], right_side[...].reshape(-1, s_width))
        egrads[c][...] = product
        add_squares(product)

    todo = list(dest_order)
    for k in range(1, n_narrow):
        for c in range(chunks):
            hidden_step(k, c)
            if k == 1 and c >= 3 and (c - 3) % 2 == 0 and len(todo) > 2:
                d = todo.pop(0)
                make_part(d)
                originate(d)
            if k == 2 and c == 1:
                while todo:
                    make_part(todo.pop(0))
                for d in dest_order[2:]:
                    if d > 0:

                        @pl.when(ni == 0)
                        def _(d=d):
                            sum_send(0, d, True)

                for d in dest_order[:1:-1]:
                    if d < last:

                        @pl.when(ni == last)
                        def _(d=d):
                            sum_send(last, d, False)

                vgrad[...] = part[ni].astype(F32)
            if k == 2 and c == 3:
                for j in range(1, n_narrow):
                    r = lax.rem(ni + n_narrow - j, n_narrow)
                    slot_arrival(r, wi).wait_recv()
                    for m in range(1, n_wide):
                        slot_relay(r, m).start()
            if k == 2 and c == chunks - 1:
                sum_slot(0)
                for copy in own_hidden:
                    copy.wait()
                for j in range(n_narrow):
                    for m in range(1, n_wide):
                        slot_arrival(j, lax.rem(wi + m, n_wide)).wait_recv()
            if k == 3:
                expert_chunk(c)
                if c % 2 == 1:
                    sum_slot(1 + c // 2)
    sum_slot(2 * (last - 1))

    def sum_out(p):
        peer = lax.rem((si * n_wide + wi) * n_narrow + ni + p, n_devices)
        device = (
            lax.div(peer, n_wide * n_narrow),
            lax.rem(lax.div(peer, n_narrow), n_wide),
            lax.rem(peer, n_narrow),
        )
        return remote(own_sum, sums.at[p], g_send.at[p], g_recv.at[p], device)

    own_sum[...] = jnp.sum(mine[...], axis=0, keepdims=True)
    sums[0] = own_sum[...]
    lax.fori_loop(1, n_devices, lambda p, _: [sum_out(p).start()] and 0, 0)
    for c in range(chunks):
        for k in range(n_narrow):

            @pl.when((ni >= k) & (ni < last))
            def _(k=k, c=c):
                hidden_copy(ni - k, c, True, False).wait_send()

            @pl.when((ni + k <= last) & (ni > 0))
            def _(k=k, c=c):
                hidden_copy(ni + k, c, False, False).wait_send()
    for copy in own_weights:
        copy.start()

    for k in range(1, n_wide):
        wide_vc(k, wi).wait_send()
        for d in range(n_narrow):
            wide_rows(k, d, wi).wait_send()
        for r in range(n_narrow):
            slot_relay(r, k).wait_send()
    for k in range(1, n_narrow):
        slot_copy(k).wait_send()
    for d in range(n_narrow):
        for q in range(RS_PIECES):

            @pl.when(ni < d)
            def _(d=d, q=q):
                sum_copy(d, q, True, False).wait_send()

            @pl.when(ni > d)
            def _(d=d, q=q):
                sum_copy(d, q, False, False).wait_send()
    for copy in own_moment:
        copy.wait()
    lax.fori_loop(1, n_devices, lambda p, _: [sum_out(p).wait_send()] and 0, 0)
    lax.fori_loop(1, n_devices, lambda p, _: [sum_out(p).wait_recv()] and 0, 0)
    total[...] = jnp.zeros_like(total) + jnp.sum(sums[...])
    for copy in own_weights:
        copy.wait()


def update_kernel(entries, chunks, split, slots, total, vgrad, *refs):
    egrads, emoms, refs = refs[:chunks], refs[chunks : 2 * chunks], refs[2 * chunks :]
    run_update(entries, split, slots, total, vgrad, egrads, emoms, refs[:chunks], *refs[chunks:])


def run_update(
    entries,
    split,
    slots,
    total,
    vgrad,
    egrads,
    emoms,
    weights,
    vm_ref,
    vw_ref,
    ew_out,
    em_out,
    vw_out,
    vm_out,
    vmom,
    vweights,
    em_stage,
    ew_stage,
    vm_stage,
    vw_stage,
    out_sem,
    v_sem,
):
    tile = egrads[0].shape[0] // split
    tiles = len(egrads) * split

    c_width = weights[0].shape[1]

    def out(t):
        rs = pl.ds(t * tile, tile)
        slot = t % slots
        return (
            pltpu.make_async_copy(em_stage.at[slot], em_out.at[rs], out_sem.at[slot, 0]),
            pltpu.make_async_copy(ew_stage.at[slot], ew_out.at[rs], out_sem.at[slot, 1]),
        )

    v_in = (
        pltpu.make_async_copy(vm_ref, vmom, v_sem.at[0]),
        pltpu.make_async_copy(vw_ref, vweights, v_sem.at[1]),
    )
    v_out = (
        pltpu.make_async_copy(vm_stage, vm_out, v_sem.at[2]),
        pltpu.make_async_copy(vw_stage, vw_out, v_sem.at[3]),
    )
    for copy in v_in:
        copy.start()
    factor = jnp.minimum(1.0, math.sqrt(entries) / jnp.sqrt(total[0:1, 0:1] + 1e-06))
    for t in range(tiles):
        slot = t % slots
        if t >= slots:
            for copy in out(t - slots):
                copy.wait()
        c, row = t // split, t % split * tile
        inner = pl.ds(row, tile)
        for j in range(em_stage.shape[2] // c_width):
            cols = pl.ds(j * c_width, c_width)
            moment = MOMENTUM_DECAY * emoms[c][inner, cols] + factor * egrads[c][inner, cols]
            weight = weights[c][pl.ds(j * c_width + row, tile)]
            em_stage[slot, :, cols] = moment
            ew_stage[slot, :, cols] = (weight.astype(F32) - STEP_RATE * moment).astype(BF16)
        for copy in out(t):
            copy.start()
    for copy in v_in:
        copy.wait()
    moment = MOMENTUM_DECAY * vmom[...] + factor * vgrad[...]
    vm_stage[...] = moment
    vw_stage[...] = (vweights[...].astype(F32) - STEP_RATE * moment).astype(BF16)
    for copy in v_out:
        copy.start()
    for t in range(max(tiles - slots, 0), tiles):
        for copy in out(t):
            copy.wait()
    for copy in v_out:
        copy.wait()


def on_device(
    normed_inputs,
    value_cotangent,
    expert_hidden,
    expert_cotangent,
    slot_gate,
    slot_count,
    expert_weight,
    expert_moment,
    value_weight,
    value_moment,
):
    n_section = lax.axis_size("section")
    n_wide = lax.axis_size("wide")
    n_narrow = lax.axis_size("narrow")
    width, kv = normed_inputs.shape[-1], value_cotangent.shape[-1]
    x = normed_inputs.reshape(-1, width)
    vc = value_cotangent.reshape(-1, kv)
    hidden = expert_hidden.reshape(-1, expert_hidden.shape[-1])
    cotangent = expert_cotangent[0, 0]
    micro, slots, _ = cotangent.shape
    in_hbm = functools.partial(pltpu.with_memory_space_constraint, memory_space=pltpu.HBM)
    tokens = x.shape[0]
    h_rows, ff = hidden.shape
    chunks = column_chunks(ff)
    r_width = width // (n_wide * n_narrow)
    s_width = width // n_narrow
    piece = RS_PIECES
    n_devices = n_section * n_wide * n_narrow
    dma = pltpu.SemaphoreType.DMA
    hbm = pl.BlockSpec(memory_space=pltpu.HBM)
    vmem = pl.BlockSpec(memory_space=pltpu.VMEM)
    block = pltpu.VMEM((ff // chunks, s_width), F32)
    w_block = pltpu.VMEM((n_narrow * h_rows, ff // chunks), BF16)
    scratch = [
        pltpu.VMEM((n_narrow, micro, n_wide, slots, s_width), BF16),
        pltpu.VMEM((micro, slots, width), BF16),
        pltpu.VMEM((n_narrow, n_wide * tokens, r_width), BF16),
        pltpu.VMEM((n_wide * tokens, kv), BF16),
        pltpu.VMEM((n_narrow, r_width, kv), BF16),
        pltpu.VMEM((n_narrow, r_width, kv), BF16),
        pltpu.VMEM((r_width, kv), BF16),
        pltpu.VMEM((n_devices, 1, 128), F32),
        pltpu.VMEM((1, 128), F32),
        pltpu.VMEM((8, 128), F32),
    ]
    *blocks, vgrad, total = pl.pallas_call(
        functools.partial(gather_kernel, (n_section, n_wide, n_narrow, chunks)),
        out_shape=(
            *[block] * (2 * chunks),
            *[w_block] * chunks,
            pltpu.VMEM((r_width, kv), F32),
            pltpu.VMEM((8, 128), F32),
        ),
        in_specs=[hbm, hbm, hbm, hbm, vmem, vmem, hbm, hbm],
        out_specs=(vmem,) * (3 * chunks + 2),
        scratch_shapes=[
            *scratch,
            dma((n_narrow, chunks)),
            dma((n_narrow, chunks)),
            dma((n_narrow, chunks)),
            dma((n_narrow, n_wide)),
            dma((n_narrow,)),
            dma((n_narrow, n_wide)),
            dma((n_wide, n_narrow + 1)),
            dma((n_wide, n_narrow + 1)),
            dma((n_narrow, piece)),
            dma((piece,)),
            dma((n_narrow, piece)),
            dma((n_narrow, piece)),
            dma((n_devices,)),
            dma((n_devices,)),
            dma((2 + n_narrow + (2 + s_width * chunks // ff) * chunks,)),
        ],
        compiler_params=pltpu.CompilerParams(
            collective_id=0, has_side_effects=True, vmem_limit_bytes=grant(scratch)
        ),
    )(
        *(in_hbm(a) for a in (x, vc, hidden, cotangent)),
        slot_gate[0, 0],
        slot_count[0],
        in_hbm(expert_moment[0]),
        in_hbm(expert_weight[0]),
    )

    total, vgrad, *blocks = (
        pltpu.with_memory_space_constraint(a, pltpu.VMEM) for a in (total, vgrad, *blocks)
    )
    layer_entries = ff * s_width + r_width * kv
    entries = n_section * n_wide * n_narrow * layer_entries
    split, depth = 2, 4
    tiles = chunks * split
    tile = ff // tiles
    update_scratch = [
        pltpu.VMEM((r_width, kv), F32),
        pltpu.VMEM((r_width, kv), BF16),
        pltpu.VMEM((depth, tile, s_width), F32),
        pltpu.VMEM((depth, tile, s_width), BF16),
        pltpu.VMEM((r_width, kv), F32),
        pltpu.VMEM((r_width, kv), BF16),
    ]
    outs = pl.pallas_call(
        functools.partial(update_kernel, entries, chunks, split, depth),
        out_shape=(
            jax.ShapeDtypeStruct((ff, s_width), BF16),
            jax.ShapeDtypeStruct((ff, s_width), F32),
            jax.ShapeDtypeStruct((r_width, kv), BF16),
            jax.ShapeDtypeStruct((r_width, kv), F32),
        ),
        in_specs=[vmem] * (3 * chunks + 2) + [hbm] * 2,
        out_specs=(hbm, hbm, hbm, hbm),
        scratch_shapes=[
            *update_scratch,
            dma((depth, 2)),
            dma((4,)),
        ],
        compiler_params=pltpu.CompilerParams(vmem_limit_bytes=grant(update_scratch)),
    )(total, vgrad, *blocks, *(in_hbm(a[0]) for a in (value_moment, value_weight)))
    return tuple(o[None] for o in outs)


def solution(mesh):
    return jax.shard_map(
        on_device,
        mesh=mesh,
        in_specs=(
            P("section", "narrow", None, "wide", None),
            P("section", "narrow", None, "wide", None),
            P("section", "narrow", None, None, "wide"),
            P("section", "narrow", None, "wide", None),
            P("section", "narrow", None, "wide"),
            P("section", "narrow", None),
            P("section", "wide", "narrow"),
            P("section", "wide", "narrow"),
            P("section", ("wide", "narrow"), None),
            P("section", ("wide", "narrow"), None),
        ),
        out_specs=(
            P("section", "wide", "narrow"),
            P("section", "wide", "narrow"),
            P("section", ("wide", "narrow"), None),
            P("section", ("wide", "narrow"), None),
        ),
        check_vma=False,
    )
```

```python
import functools
import math

import jax
import jax.numpy as jnp
from jax import lax
from jax.experimental import pallas as pl
from jax.experimental.pallas import tpu as pltpu
from jax.sharding import PartitionSpec as P

MOMENTUM_DECAY = 0.9
STEP_RATE = 0.01
MESH = pl.DeviceIdType.MESH
F32 = jnp.float32
BF16 = jnp.bfloat16
RS_PIECES = 4


def column_chunks(width):
    lanes = width // 128
    return max(c for c in range(1, 9) if lanes % c == 0)


def grant(scratch, *arrays):
    held = [(math.prod(a.shape), a.dtype) for a in arrays]
    held += [(math.prod(a.inner_aval.shape), a.inner_aval.dtype) for a in scratch]
    return sum(n * d.itemsize for n, d in held) + 4 * 2**20


def dot_rows(a, b):
    return lax.dot_general(a, b, (((0,), (0,)), ((), ())), preferred_element_type=F32)


def gather_kernel(
    dims,
    x_ref,
    vc_ref,
    h_ref,
    cot_ref,
    gate_ref,
    count_ref,
    mom_ref,
    w_ref,
    *refs,
):
    n_section, n_wide, n_narrow, chunks = dims
    arrays = (x_ref, vc_ref, h_ref, cot_ref, gate_ref, count_ref, mom_ref, w_ref)
    egrads, emoms, refs = refs[:chunks], refs[chunks : 2 * chunks], refs[2 * chunks :]
    run_gather(dims, *arrays, egrads, emoms, refs[:chunks], *refs[chunks:])


def run_gather(
    dims,
    x_ref,
    vc_ref,
    h_ref,
    cot_ref,
    gate_ref,
    count_ref,
    mom_ref,
    w_ref,
    egrads,
    emoms,
    hbuf,
    vgrad,
    total,
    sbuf,
    scaled,
    rows,
    cots,
    part,
    rbuf,
    rlast,
    sums,
    own_sum,
    mine,
    h_recv,
    h_right,
    h_left,
    s_recv,
    s_send,
    s_relay,
    x_recv,
    x_send,
    r_recv,
    r_last,
    r_right,
    r_left,
    g_recv,
    g_send,
    local,
    p_recv,
    p_send,
    spare,
):
    n_section, n_wide, n_narrow, chunks = dims
    si, wi, ni = lax.axis_index("section"), lax.axis_index("wide"), lax.axis_index("narrow")
    last = n_narrow - 1
    tokens = x_ref.shape[0]
    h_rows = h_ref.shape[0]
    c_width = h_ref.shape[1] // chunks
    r_width = rows.shape[2]
    s_width = sbuf.shape[4]
    piece = r_width // RS_PIECES
    dest_order = [d for pair in zip(range(last, -1, -1), range(n_narrow)) for d in pair]
    dest_order = list(dict.fromkeys(dest_order))

    def at(section=0, wide=0, narrow=0):
        return (
            lax.rem(si + section, n_section),
            lax.rem(wi + wide, n_wide),
            lax.rem(ni + narrow, n_narrow),
        )

    def remote(src, dst, send_sem, recv_sem, device):
        return pltpu.make_async_remote_copy(
            src_ref=src,
            dst_ref=dst,
            send_sem=send_sem,
            recv_sem=recv_sem,
            device_id=device,
            device_id_type=MESH,
        )

    right, left = (si, wi, jnp.minimum(ni + 1, last)), (si, wi, jnp.maximum(ni - 1, 0))
    n_devices = n_section * n_wide * n_narrow
    greeted = [(s, 0, 0) for s in range(1, n_section)]
    greeted += [(0, w, 0) for w in range(1, n_wide)]
    greeted += [(0, 0, n) for n in range(1, n_narrow)]

    barrier = pltpu.get_barrier_semaphore()
    for offset in greeted:
        pl.semaphore_signal(barrier, inc=1, device_id=at(*offset), device_id_type=MESH)

    own = []
    own.append(
        pltpu.make_async_copy(vc_ref, cots.at[pl.ds(wi * tokens, tokens)], local.at[0])
    )
    for d in range(n_narrow):
        start = pl.multiple_of((wi * n_narrow + d) * r_width, r_width)
        own.append(
            pltpu.make_async_copy(
                x_ref.at[:, pl.ds(start, r_width)],
                rows.at[d, pl.ds(wi * tokens, tokens)],
                local.at[1 + d],
            )
        )
    own_hidden = [
        pltpu.make_async_copy(
            h_ref.at[:, pl.ds(c * c_width, c_width)],
            hbuf[c].at[pl.ds(ni * h_rows, h_rows)],
            local.at[1 + n_narrow + c],
        )
        for c in range(chunks)
    ]
    own_moment = [
        pltpu.make_async_copy(
            mom_ref.at[pl.ds(c * c_width, c_width)],
            emoms[c],
            local.at[1 + n_narrow + chunks + c],
        )
        for c in range(chunks)
    ]
    own_slots = pltpu.make_async_copy(cot_ref, scaled, local.at[1 + n_narrow + 2 * chunks])
    blocks = s_width // c_width
    own_weights = [
        pltpu.make_async_copy(
            w_ref.at[pl.ds(c * c_width, c_width), pl.ds(j * c_width, c_width)],
            hbuf[c].at[pl.ds(j * c_width, c_width)],
            local.at[2 + n_narrow + 2 * chunks + c * blocks + j],
        )
        for c in range(chunks)
        for j in range(blocks)
    ]
    for copy in [own_slots] + own + own_hidden:
        copy.start()

    pl.semaphore_wait(barrier, len(greeted))

    def hidden_copy(r, c, rightward, first):
        block = hbuf[c].at[pl.ds(r * h_rows, h_rows)]
        src = h_ref.at[:, pl.ds(c * c_width, c_width)] if first else block
        sems = h_right if rightward else h_left
        return remote(src, block, sems.at[c], h_recv.at[r, c], right if rightward else left)

    def send_own_hidden(c):
        @pl.when(ni < last)
        def _():
            hidden_copy(ni, c, True, True).start()

        @pl.when(ni > 0)
        def _():
            hidden_copy(ni, c, False, True).start()

    def hidden_step(k, c):
        @pl.when(ni >= k)
        def _():
            hidden_copy(ni - k, c, True, False).wait_recv()

            @pl.when(ni < last)
            def _():
                hidden_copy(ni - k, c, True, False).start()

        @pl.when(ni + k <= last)
        def _():
            hidden_copy(ni + k, c, False, False).wait_recv()

            @pl.when(ni > 0)
            def _():
                hidden_copy(ni + k, c, False, False).start()

    def wide_vc(k, source):
        return remote(
            vc_ref,
            cots.at[pl.ds(source * tokens, tokens)],
            x_send.at[k, n_narrow],
            x_recv.at[source, n_narrow],
            at(0, k, 0),
        )

    def wide_rows(k, d, source):
        peer = lax.rem(wi + k, n_wide)
        start = pl.multiple_of((peer * n_narrow + d) * r_width, r_width)
        return remote(
            x_ref.at[:, pl.ds(start, r_width)],
            rows.at[d, pl.ds(source * tokens, tokens)],
            x_send.at[k, d],
            x_recv.at[source, d],
            at(0, k, 0),
        )

    def slot_copy(k):
        peer = lax.rem(ni + k, n_narrow)
        start = pl.multiple_of(peer * s_width, s_width)
        return remote(
            scaled.at[:, :, pl.ds(start, s_width)],
            sbuf.at[ni, :, wi],
            s_send.at[k],
            s_recv.at[ni, wi],
            at(0, 0, k),
        )

    def slot_relay(r, k):
        return remote(
            sbuf.at[r, :, wi],
            sbuf.at[r, :, wi],
            s_relay.at[r, k],
            s_recv.at[r, wi],
            at(0, k, 0),
        )

    def slot_arrival(r, w):
        return remote(sbuf.at[r, :, w], sbuf.at[r, :, w], s_send.at[0], s_recv.at[r, w], right)

    for c in range(0, 2):
        send_own_hidden(c)
    for k in range(1, n_wide):
        wide_vc(k, wi).start()
    for d in dest_order:
        for k in range(1, n_wide):
            wide_rows(k, d, wi).start()

    own_slots.wait()
    slots = scaled.shape[1]
    down = lax.broadcasted_iota(jnp.int32, (slots, slots), 0)
    across = lax.broadcasted_iota(jnp.int32, (slots, slots), 1)
    for m in range(scaled.shape[0]):
        live = wi * slots + across < count_ref[0:1, m : m + 1]
        gates = jnp.where(live & (down == across), gate_ref[m : m + 1, :].astype(F32), 0.0)
        coefficient = jnp.sum(gates, axis=1, keepdims=True)
        scaled[m] = (coefficient * scaled[m].astype(F32)).astype(BF16)
    for k in range(1, n_narrow):
        slot_copy(k).start()
    for c in range(2, chunks):
        send_own_hidden(c)
    for copy in own_moment:
        copy.start()
    own_start = pl.multiple_of(ni * s_width, s_width)
    sbuf[ni, :, wi] = scaled[:, :, pl.ds(own_start, s_width)]
    for k in range(1, n_wide):
        slot_relay(ni, k).start()

    def make_part(d):
        if d == dest_order[0]:
            own[0].wait()
            for k in range(1, n_wide):
                wide_vc(k, lax.rem(wi + n_wide - k, n_wide)).wait_recv()
        own[1 + d].wait()
        for k in range(1, n_wide):
            wide_rows(k, d, lax.rem(wi + n_wide - k, n_wide)).wait_recv()
        part[d] = dot_rows(rows[d], cots[...]).astype(BF16)

    mine[...] = jnp.zeros_like(mine)

    def add_squares(block):
        sq = block * block
        n_rows, n_cols = sq.shape
        folded = jnp.sum(sq.reshape(n_rows // 8, 8, n_cols), axis=0)
        acc = folded[:, 0:128]
        for lane in range(128, n_cols, 128):
            acc = acc + folded[:, lane : lane + 128]
        mine[...] += acc

    def piece_at(ref, d, q):
        return ref.at[d, pl.ds(q * piece, piece)]

    def sum_copy(d, q, rightward, final):
        dst = rlast.at[pl.ds(q * piece, piece)] if final else piece_at(rbuf, d, q)
        sem = r_last.at[q] if final else r_recv.at[d, q]
        sems = r_right if rightward else r_left
        return remote(piece_at(part, d, q), dst, sems.at[d], sem, right if rightward else left)

    def sum_send(i, d, rightward):
        final_right = rightward and d == i + 1
        for q in range(RS_PIECES):
            sum_copy(d, q, rightward, final_right).start()

    def sum_slot(slot):
        for i in range(1, n_narrow):
            j = slot - 2 * (i - 1)
            if j < 0 or j > last - i:
                continue
            for rightward in (True, False):
                me = i if rightward else last - i
                d = last - j if rightward else j

                @pl.when(ni == me)
                def _(me=me, d=d, rightward=rightward):
                    final = d == me
                    landing = final and rightward
                    for q in range(RS_PIECES):
                        sum_copy(d, q, rightward, landing).wait_recv()
                        rs = pl.ds(q * piece, piece)
                        came = rlast[rs] if landing else rbuf[d, rs]
                        if final:
                            done = vgrad[rs] + came.astype(F32)
                            vgrad[rs] = done
                            if me not in (0, last) and rightward == (2 * me > last):
                                add_squares(done)
                        else:
                            part[d, rs] = (part[d, rs].astype(F32) + came.astype(F32)).astype(BF16)
                            ahead = me + 1 if rightward else me - 1
                            if ahead not in (0, last) or q < RS_PIECES - 1:
                                sum_copy(d, q, rightward, rightward and d == ahead).start()

    def edge_part(rightward):
        return remote(
            part.at[0 if rightward else last],
            cots.at[pl.ds(0, r_width)],
            p_send.at[0],
            p_recv.at[0],
            right if rightward else left,
        )

    def grant_spare():
        @pl.when(ni == 1)
        def _():
            pl.semaphore_signal(spare, inc=1, device_id=left, device_id_type=MESH)

        @pl.when(ni == last - 1)
        def _():
            pl.semaphore_signal(spare, inc=1, device_id=right, device_id_type=MESH)

    def send_edge_part():
        for edge in (0, last):

            @pl.when(ni == edge)
            def _(edge=edge):
                pl.semaphore_wait(spare, 1)
                edge_part(edge == 0).start()

    def edge_squares():
        for me, d in ((1, 0), (last - 1, last)):

            @pl.when(ni == me)
            def _(d=d):
                edge_part(d == 0).wait_recv()
                for q in range(RS_PIECES):
                    rs = pl.ds(q * piece, piece)
                    add_squares(part[d, rs].astype(F32) + cots[rs].astype(F32))

    def originate(d):
        if d > 0:

            @pl.when(ni == 0)
            def _():
                sum_send(0, d, True)

        if d < last:

            @pl.when(ni == last)
            def _():
                sum_send(last, d, False)

    right_side = sbuf.at[...]

    def expert_chunk(c):
        product = dot_rows(hbuf[c][...], right_side[...].reshape(-1, s_width))
        egrads[c][...] = product
        add_squares(product)

    todo = list(dest_order)
    for k in range(1, n_narrow):
        for c in range(chunks):
            hidden_step(k, c)
            if k == 1 and c >= 3 and (c - 3) % 2 == 0 and len(todo) > 2:
                d = todo.pop(0)
                make_part(d)
                originate(d)
            if k == 2 and c == 1:
                while todo:
                    make_part(todo.pop(0))
                for d in dest_order[2:]:
                    if d > 0:

                        @pl.when(ni == 0)
                        def _(d=d):
                            sum_send(0, d, True)

                for d in dest_order[:1:-1]:
                    if d < last:

                        @pl.when(ni == last)
                        def _(d=d):
                            sum_send(last, d, False)

                grant_spare()
                vgrad[...] = part[ni].astype(F32)
            if k == 2 and c == 3:
                send_edge_part()
                for j in range(1, n_narrow):
                    r = lax.rem(ni + n_narrow - j, n_narrow)
                    slot_arrival(r, wi).wait_recv()
                    for m in range(1, n_wide):
                        slot_relay(r, m).start()
            if k == 2 and c == chunks - 1:
                sum_slot(0)
                for copy in own_hidden:
                    copy.wait()
                for j in range(n_narrow):
                    for m in range(1, n_wide):
                        slot_arrival(j, lax.rem(wi + m, n_wide)).wait_recv()
            if k == 3:
                expert_chunk(c)
                if c % 2 == 1:
                    sum_slot(1 + c // 2)
    edge_squares()

    def sum_out(p):
        peer = lax.rem((si * n_wide + wi) * n_narrow + ni + p, n_devices)
        device = (
            lax.div(peer, n_wide * n_narrow),
            lax.rem(lax.div(peer, n_narrow), n_wide),
            lax.rem(peer, n_narrow),
        )
        return remote(own_sum, sums.at[p], g_send.at[0], g_recv.at[0], device)

    def all_sums():
        others = sums.at[pl.ds(1, n_devices - 1)]
        return remote(others, others, g_send.at[0], g_recv.at[0], right)

    own_sum[...] = jnp.sum(mine[...], axis=0, keepdims=True)
    sums[0] = own_sum[...]
    lax.fori_loop(1, n_devices, lambda p, _: [sum_out(p).start()] and 0, 0)
    for me, d in ((1, 0), (last - 1, last)):

        @pl.when(ni == me)
        def _(d=d):
            sum_copy(d, RS_PIECES - 1, d == last, d == last).start()

    for i in range(n_narrow):

        @pl.when(ni == i)
        def _(i=i):
            for c in range(chunks):
                for rightward in (True, False):
                    n_sent = i + 1 if rightward else n_narrow - i
                    if i == (last if rightward else 0):
                        continue
                    sent = hbuf[c].at[pl.ds(0, n_sent * h_rows)]
                    sem = (h_right if rightward else h_left).at[c]
                    remote(sent, sent, sem, h_recv.at[0, c], right).wait_send()

    for copy in own_weights:
        copy.start()

    for edge in (0, last):

        @pl.when(ni == edge)
        def _(edge=edge):
            edge_part(edge == 0).wait_send()

    for k in range(1, n_wide):
        wide_vc(k, wi).wait_send()
        for d in range(n_narrow):
            wide_rows(k, d, wi).wait_send()
        for r in range(n_narrow):
            slot_relay(r, k).wait_send()
    for k in range(1, n_narrow):
        slot_copy(k).wait_send()
    for d in range(n_narrow):

        @pl.when(ni < d)
        def _(d=d):
            remote(part.at[d], rbuf.at[d], r_right.at[d], r_last.at[0], right).wait_send()

        @pl.when(ni > d)
        def _(d=d):
            remote(part.at[d], rbuf.at[d], r_left.at[d], r_last.at[0], left).wait_send()

    for copy in own_moment:
        copy.wait()
    for copy in own_weights:
        copy.wait()
    all_sums().wait_send()
    sum_slot(2 * (last - 1))
    all_sums().wait_recv()
    total[...] = jnp.zeros_like(total) + jnp.sum(sums[...])


def update_kernel(entries, chunks, split, slots, total, vgrad, *refs):
    egrads, emoms, refs = refs[:chunks], refs[chunks : 2 * chunks], refs[2 * chunks :]
    run_update(entries, split, slots, total, vgrad, egrads, emoms, refs[:chunks], *refs[chunks:])


def run_update(
    entries,
    split,
    slots,
    total,
    vgrad,
    egrads,
    emoms,
    weights,
    vm_ref,
    vw_ref,
    ew_out,
    em_out,
    vw_out,
    vm_out,
    vmom,
    vweights,
    em_stage,
    ew_stage,
    vm_stage,
    vw_stage,
    out_sem,
    v_sem,
):
    tile = egrads[0].shape[0] // split
    tiles = len(egrads) * split

    c_width = weights[0].shape[1]

    def out(t):
        rs = pl.ds(t * tile, tile)
        slot = t % slots
        return (
            pltpu.make_async_copy(em_stage.at[slot], em_out.at[rs], out_sem.at[slot, 0]),
            pltpu.make_async_copy(ew_stage.at[slot], ew_out.at[rs], out_sem.at[slot, 1]),
        )

    v_in = (
        pltpu.make_async_copy(vm_ref, vmom, v_sem.at[0]),
        pltpu.make_async_copy(vw_ref, vweights, v_sem.at[1]),
    )
    v_out = (
        pltpu.make_async_copy(vm_stage, vm_out, v_sem.at[2]),
        pltpu.make_async_copy(vw_stage, vw_out, v_sem.at[3]),
    )
    for copy in v_in:
        copy.start()
    factor = jnp.minimum(1.0, math.sqrt(entries) / jnp.sqrt(total[0:1, 0:1] + 1e-06))
    for t in range(tiles):
        slot = t % slots
        if t >= slots:
            for copy in out(t - slots):
                copy.wait()
        c, row = t // split, t % split * tile
        inner = pl.ds(row, tile)
        for j in range(em_stage.shape[2] // c_width):
            cols = pl.ds(j * c_width, c_width)
            moment = MOMENTUM_DECAY * emoms[c][inner, cols] + factor * egrads[c][inner, cols]
            weight = weights[c][pl.ds(j * c_width + row, tile)]
            em_stage[slot, :, cols] = moment
            ew_stage[slot, :, cols] = (weight.astype(F32) - STEP_RATE * moment).astype(BF16)
        for copy in out(t):
            copy.start()
    for copy in v_in:
        copy.wait()
    moment = MOMENTUM_DECAY * vmom[...] + factor * vgrad[...]
    vm_stage[...] = moment
    vw_stage[...] = (vweights[...].astype(F32) - STEP_RATE * moment).astype(BF16)
    for copy in v_out:
        copy.start()
    for t in range(max(tiles - slots, 0), tiles):
        for copy in out(t):
            copy.wait()
    for copy in v_out:
        copy.wait()


def on_device(
    normed_inputs,
    value_cotangent,
    expert_hidden,
    expert_cotangent,
    slot_gate,
    slot_count,
    expert_weight,
    expert_moment,
    value_weight,
    value_moment,
):
    n_section = lax.axis_size("section")
    n_wide = lax.axis_size("wide")
    n_narrow = lax.axis_size("narrow")
    width, kv = normed_inputs.shape[-1], value_cotangent.shape[-1]
    x = normed_inputs.reshape(-1, width)
    vc = value_cotangent.reshape(-1, kv)
    hidden = expert_hidden.reshape(-1, expert_hidden.shape[-1])
    cotangent = expert_cotangent[0, 0]
    micro, slots, _ = cotangent.shape
    in_hbm = functools.partial(pltpu.with_memory_space_constraint, memory_space=pltpu.HBM)
    tokens = x.shape[0]
    h_rows, ff = hidden.shape
    chunks = column_chunks(ff)
    r_width = width // (n_wide * n_narrow)
    s_width = width // n_narrow
    piece = RS_PIECES
    n_devices = n_section * n_wide * n_narrow
    dma = pltpu.SemaphoreType.DMA
    hbm = pl.BlockSpec(memory_space=pltpu.HBM)
    vmem = pl.BlockSpec(memory_space=pltpu.VMEM)
    block = pltpu.VMEM((ff // chunks, s_width), F32)
    w_block = pltpu.VMEM((n_narrow * h_rows, ff // chunks), BF16)
    scratch = [
        pltpu.VMEM((n_narrow, micro, n_wide, slots, s_width), BF16),
        pltpu.VMEM((micro, slots, width), BF16),
        pltpu.VMEM((n_narrow, n_wide * tokens, r_width), BF16),
        pltpu.VMEM((n_wide * tokens, kv), BF16),
        pltpu.VMEM((n_narrow, r_width, kv), BF16),
        pltpu.VMEM((n_narrow, r_width, kv), BF16),
        pltpu.VMEM((r_width, kv), BF16),
        pltpu.VMEM((n_devices, 1, 128), F32),
        pltpu.VMEM((1, 128), F32),
        pltpu.VMEM((8, 128), F32),
    ]
    *blocks, vgrad, total = pl.pallas_call(
        functools.partial(gather_kernel, (n_section, n_wide, n_narrow, chunks)),
        out_shape=(
            *[block] * (2 * chunks),
            *[w_block] * chunks,
            pltpu.VMEM((r_width, kv), F32),
            pltpu.VMEM((8, 128), F32),
        ),
        in_specs=[hbm, hbm, hbm, hbm, vmem, vmem, hbm, hbm],
        out_specs=(vmem,) * (3 * chunks + 2),
        scratch_shapes=[
            *scratch,
            dma((n_narrow, chunks)),
            dma((chunks,)),
            dma((chunks,)),
            dma((n_narrow, n_wide)),
            dma((n_narrow,)),
            dma((n_narrow, n_wide)),
            dma((n_wide, n_narrow + 1)),
            dma((n_wide, n_narrow + 1)),
            dma((n_narrow, piece)),
            dma((piece,)),
            dma((n_narrow,)),
            dma((n_narrow,)),
            dma((1,)),
            dma((1,)),
            dma((2 + n_narrow + (2 + s_width * chunks // ff) * chunks,)),
            dma((1,)),
            dma((1,)),
            pltpu.SemaphoreType.REGULAR,
        ],
        compiler_params=pltpu.CompilerParams(
            collective_id=0, has_side_effects=True, vmem_limit_bytes=grant(scratch)
        ),
    )(
        *(in_hbm(a) for a in (x, vc, hidden, cotangent)),
        slot_gate[0, 0],
        slot_count[0],
        in_hbm(expert_moment[0]),
        in_hbm(expert_weight[0]),
    )

    total, vgrad, *blocks = (
        pltpu.with_memory_space_constraint(a, pltpu.VMEM) for a in (total, vgrad, *blocks)
    )
    layer_entries = ff * s_width + r_width * kv
    entries = n_section * n_wide * n_narrow * layer_entries
    split, depth = 2, 4
    tiles = chunks * split
    tile = ff // tiles
    update_scratch = [
        pltpu.VMEM((r_width, kv), F32),
        pltpu.VMEM((r_width, kv), BF16),
        pltpu.VMEM((depth, tile, s_width), F32),
        pltpu.VMEM((depth, tile, s_width), BF16),
        pltpu.VMEM((r_width, kv), F32),
        pltpu.VMEM((r_width, kv), BF16),
    ]
    outs = pl.pallas_call(
        functools.partial(update_kernel, entries, chunks, split, depth),
        out_shape=(
            jax.ShapeDtypeStruct((ff, s_width), BF16),
            jax.ShapeDtypeStruct((ff, s_width), F32),
            jax.ShapeDtypeStruct((r_width, kv), BF16),
            jax.ShapeDtypeStruct((r_width, kv), F32),
        ),
        in_specs=[vmem] * (3 * chunks + 2) + [hbm] * 2,
        out_specs=(hbm, hbm, hbm, hbm),
        scratch_shapes=[
            *update_scratch,
            dma((depth, 2)),
            dma((4,)),
        ],
        compiler_params=pltpu.CompilerParams(vmem_limit_bytes=grant(update_scratch)),
    )(total, vgrad, *blocks, *(in_hbm(a[0]) for a in (value_moment, value_weight)))
    return tuple(o[None] for o in outs)


def solution(mesh):
    return jax.shard_map(
        on_device,
        mesh=mesh,
        in_specs=(
            P("section", "narrow", None, "wide", None),
            P("section", "narrow", None, "wide", None),
            P("section", "narrow", None, None, "wide"),
            P("section", "narrow", None, "wide", None),
            P("section", "narrow", None, "wide"),
            P("section", "narrow", None),
            P("section", "wide", "narrow"),
            P("section", "wide", "narrow"),
            P("section", ("wide", "narrow"), None),
            P("section", ("wide", "narrow"), None),
        ),
        out_specs=(
            P("section", "wide", "narrow"),
            P("section", "wide", "narrow"),
            P("section", ("wide", "narrow"), None),
            P("section", ("wide", "narrow"), None),
        ),
        check_vma=False,
    )
```

```python
import functools
import math

import jax
import jax.numpy as jnp
from jax import lax
from jax.experimental import pallas as pl
from jax.experimental.pallas import tpu as pltpu
from jax.sharding import PartitionSpec as P

MOMENTUM_DECAY = 0.9
STEP_RATE = 0.01
MESH = pl.DeviceIdType.MESH
F32 = jnp.float32
BF16 = jnp.bfloat16
RS_PIECES = 4


def column_chunks(width):
    lanes = width // 128
    return max(c for c in range(1, 9) if lanes % c == 0)


def grant(scratch, *arrays):
    held = [(math.prod(a.shape), a.dtype) for a in arrays]
    held += [(math.prod(a.inner_aval.shape), a.inner_aval.dtype) for a in scratch]
    return sum(n * d.itemsize for n, d in held) + 4 * 2**20


def dot_rows(a, b):
    return lax.dot_general(a, b, (((0,), (0,)), ((), ())), preferred_element_type=F32)


def gather_kernel(
    dims,
    x_ref,
    vc_ref,
    h_ref,
    cot_ref,
    gate_ref,
    count_ref,
    mom_ref,
    w_ref,
    *refs,
):
    n_section, n_wide, n_narrow, chunks = dims
    arrays = (x_ref, vc_ref, h_ref, cot_ref, gate_ref, count_ref, mom_ref, w_ref)
    egrads, emoms, refs = refs[:chunks], refs[chunks : 2 * chunks], refs[2 * chunks :]
    run_gather(dims, *arrays, egrads, emoms, refs[:chunks], *refs[chunks:])


def run_gather(
    dims,
    x_ref,
    vc_ref,
    h_ref,
    cot_ref,
    gate_ref,
    count_ref,
    mom_ref,
    w_ref,
    egrads,
    emoms,
    hbuf,
    vgrad,
    total,
    sbuf,
    scaled,
    rows,
    cots,
    part,
    rbuf,
    rlast,
    sums,
    own_sum,
    mine,
    h_recv,
    h_right,
    h_left,
    s_recv,
    s_send,
    s_relay,
    x_recv,
    x_send,
    r_recv,
    r_last,
    r_right,
    r_left,
    g_recv,
    g_send,
    local,
    p_recv,
    p_send,
    spare,
):
    n_section, n_wide, n_narrow, chunks = dims
    si, wi, ni = lax.axis_index("section"), lax.axis_index("wide"), lax.axis_index("narrow")
    last = n_narrow - 1
    tokens = x_ref.shape[0]
    h_rows = h_ref.shape[0]
    c_width = h_ref.shape[1] // chunks
    r_width = rows.shape[2]
    s_width = sbuf.shape[4]
    piece = r_width // RS_PIECES
    dest_order = [d for pair in zip(range(last, -1, -1), range(n_narrow)) for d in pair]
    dest_order = list(dict.fromkeys(dest_order))

    def at(section=0, wide=0, narrow=0):
        return (
            lax.rem(si + section, n_section),
            lax.rem(wi + wide, n_wide),
            lax.rem(ni + narrow, n_narrow),
        )

    def remote(src, dst, send_sem, recv_sem, device):
        return pltpu.make_async_remote_copy(
            src_ref=src,
            dst_ref=dst,
            send_sem=send_sem,
            recv_sem=recv_sem,
            device_id=device,
            device_id_type=MESH,
        )

    right, left = (si, wi, jnp.minimum(ni + 1, last)), (si, wi, jnp.maximum(ni - 1, 0))
    n_devices = n_section * n_wide * n_narrow
    greeted = [(s, 0, 0) for s in range(1, n_section)]
    greeted += [(0, w, 0) for w in range(1, n_wide)]
    greeted += [(0, 0, n) for n in range(1, n_narrow)]

    barrier = pltpu.get_barrier_semaphore()
    for offset in greeted:
        pl.semaphore_signal(barrier, inc=1, device_id=at(*offset), device_id_type=MESH)

    own = []
    own.append(
        pltpu.make_async_copy(vc_ref, cots.at[pl.ds(wi * tokens, tokens)], local.at[0])
    )
    for d in range(n_narrow):
        start = pl.multiple_of((wi * n_narrow + d) * r_width, r_width)
        own.append(
            pltpu.make_async_copy(
                x_ref.at[:, pl.ds(start, r_width)],
                rows.at[d, pl.ds(wi * tokens, tokens)],
                local.at[1 + d],
            )
        )
    own_hidden = [
        pltpu.make_async_copy(
            h_ref.at[:, pl.ds(c * c_width, c_width)],
            hbuf[c].at[pl.ds(ni * h_rows, h_rows)],
            local.at[1 + n_narrow + c],
        )
        for c in range(chunks)
    ]
    own_moment = [
        pltpu.make_async_copy(
            mom_ref.at[pl.ds(c * c_width, c_width)],
            emoms[c],
            local.at[1 + n_narrow + chunks + c],
        )
        for c in range(chunks)
    ]
    own_slots = pltpu.make_async_copy(cot_ref, scaled, local.at[1 + n_narrow + 2 * chunks])
    blocks = s_width // c_width
    own_weights = [
        pltpu.make_async_copy(
            w_ref.at[pl.ds(c * c_width, c_width), pl.ds(j * c_width, c_width)],
            hbuf[c].at[pl.ds(j * c_width, c_width)],
            local.at[2 + n_narrow + 2 * chunks + c * blocks + j],
        )
        for c in range(chunks)
        for j in range(blocks)
    ]
    for copy in [own_slots] + own + own_hidden:
        copy.start()

    pl.semaphore_wait(barrier, len(greeted))

    def hidden_copy(r, c, rightward, first):
        block = hbuf[c].at[pl.ds(r * h_rows, h_rows)]
        src = h_ref.at[:, pl.ds(c * c_width, c_width)] if first else block
        sems = h_right if rightward else h_left
        return remote(src, block, sems.at[c], h_recv.at[r, c], right if rightward else left)

    def send_own_hidden(c):
        @pl.when(ni < last)
        def _():
            hidden_copy(ni, c, True, True).start()

        @pl.when(ni > 0)
        def _():
            hidden_copy(ni, c, False, True).start()

    def hidden_step(k, c):
        @pl.when(ni >= k)
        def _():
            hidden_copy(ni - k, c, True, False).wait_recv()

            @pl.when(ni < last)
            def _():
                hidden_copy(ni - k, c, True, False).start()

        @pl.when(ni + k <= last)
        def _():
            hidden_copy(ni + k, c, False, False).wait_recv()

            @pl.when(ni > 0)
            def _():
                hidden_copy(ni + k, c, False, False).start()

    def wide_vc(k, source):
        return remote(
            vc_ref,
            cots.at[pl.ds(source * tokens, tokens)],
            x_send.at[k, n_narrow],
            x_recv.at[source, n_narrow],
            at(0, k, 0),
        )

    def wide_rows(k, d, source):
        peer = lax.rem(wi + k, n_wide)
        start = pl.multiple_of((peer * n_narrow + d) * r_width, r_width)
        return remote(
            x_ref.at[:, pl.ds(start, r_width)],
            rows.at[d, pl.ds(source * tokens, tokens)],
            x_send.at[k, d],
            x_recv.at[source, d],
            at(0, k, 0),
        )

    def slot_copy(k):
        peer = lax.rem(ni + k, n_narrow)
        start = pl.multiple_of(peer * s_width, s_width)
        return remote(
            scaled.at[:, :, pl.ds(start, s_width)],
            sbuf.at[ni, :, wi],
            s_send.at[k],
            s_recv.at[ni, wi],
            at(0, 0, k),
        )

    def slot_relay(r, k):
        return remote(
            sbuf.at[r, :, wi],
            sbuf.at[r, :, wi],
            s_relay.at[r, k],
            s_recv.at[r, wi],
            at(0, k, 0),
        )

    def slot_arrival(r, w):
        return remote(sbuf.at[r, :, w], sbuf.at[r, :, w], s_send.at[0], s_recv.at[r, w], right)

    for c in range(0, 2):
        send_own_hidden(c)
    for k in range(1, n_wide):
        wide_vc(k, wi).start()
    for d in dest_order:
        for k in range(1, n_wide):
            wide_rows(k, d, wi).start()

    own_slots.wait()
    slots = scaled.shape[1]
    down = lax.broadcasted_iota(jnp.int32, (slots, slots), 0)
    across = lax.broadcasted_iota(jnp.int32, (slots, slots), 1)
    for m in range(scaled.shape[0]):
        live = wi * slots + across < count_ref[0:1, m : m + 1]
        gates = jnp.where(live & (down == across), gate_ref[m : m + 1, :].astype(F32), 0.0)
        coefficient = jnp.sum(gates, axis=1, keepdims=True)
        scaled[m] = (coefficient * scaled[m].astype(F32)).astype(BF16)
    for k in range(1, n_narrow):
        slot_copy(k).start()
    for c in range(2, chunks):
        send_own_hidden(c)
    for copy in own_moment:
        copy.start()
    own_start = pl.multiple_of(ni * s_width, s_width)
    sbuf[ni, :, wi] = scaled[:, :, pl.ds(own_start, s_width)]
    for k in range(1, n_wide):
        slot_relay(ni, k).start()

    def make_part(d):
        if d == dest_order[0]:
            own[0].wait()
            for k in range(1, n_wide):
                wide_vc(k, lax.rem(wi + n_wide - k, n_wide)).wait_recv()
        own[1 + d].wait()
        for k in range(1, n_wide):
            wide_rows(k, d, lax.rem(wi + n_wide - k, n_wide)).wait_recv()
        part[d] = dot_rows(rows[d], cots[...]).astype(BF16)

    mine[...] = jnp.zeros_like(mine)

    def add_squares(block):
        sq = block * block
        n_rows, n_cols = sq.shape
        folded = jnp.sum(sq.reshape(n_rows // 8, 8, n_cols), axis=0)
        acc = folded[:, 0:128]
        for lane in range(128, n_cols, 128):
            acc = acc + folded[:, lane : lane + 128]
        mine[...] += acc

    def piece_at(ref, d, q):
        return ref.at[d, pl.ds(q * piece, piece)]

    def sum_copy(d, q, rightward, final):
        dst = rlast.at[pl.ds(q * piece, piece)] if final else piece_at(rbuf, d, q)
        sem = r_last.at[q] if final else r_recv.at[d, q]
        sems = r_right if rightward else r_left
        return remote(piece_at(part, d, q), dst, sems.at[d], sem, right if rightward else left)

    def sum_send(i, d, rightward):
        final_right = rightward and d == i + 1
        for q in range(RS_PIECES):
            sum_copy(d, q, rightward, final_right).start()

    def sum_slot(slot):
        for i in range(1, n_narrow):
            j = slot - 2 * (i - 1)
            if j < 0 or j > last - i:
                continue
            for rightward in (True, False):
                me = i if rightward else last - i
                d = last - j if rightward else j

                @pl.when(ni == me)
                def _(me=me, d=d, rightward=rightward):
                    final = d == me
                    landing = final and rightward
                    for q in range(RS_PIECES):
                        sum_copy(d, q, rightward, landing).wait_recv()
                        rs = pl.ds(q * piece, piece)
                        came = rlast[rs] if landing else rbuf[d, rs]
                        if final:
                            done = vgrad[rs] + came.astype(F32)
                            vgrad[rs] = done
                            if me not in (0, last) and rightward == (2 * me > last):
                                add_squares(done)
                        else:
                            part[d, rs] = (part[d, rs].astype(F32) + came.astype(F32)).astype(BF16)
                            ahead = me + 1 if rightward else me - 1
                            if ahead not in (0, last) or q < RS_PIECES - 1:
                                sum_copy(d, q, rightward, rightward and d == ahead).start()

    def edge_part(rightward):
        return remote(
            part.at[0 if rightward else last],
            cots.at[pl.ds(0, r_width)],
            p_send.at[0],
            p_recv.at[0],
            right if rightward else left,
        )

    def grant_spare():
        @pl.when(ni == 1)
        def _():
            pl.semaphore_signal(spare, inc=1, device_id=left, device_id_type=MESH)

        @pl.when(ni == last - 1)
        def _():
            pl.semaphore_signal(spare, inc=1, device_id=right, device_id_type=MESH)

    def send_edge_part():
        for edge in (0, last):

            @pl.when(ni == edge)
            def _(edge=edge):
                pl.semaphore_wait(spare, 1)
                edge_part(edge == 0).start()

    def edge_squares():
        for me, d in ((1, 0), (last - 1, last)):

            @pl.when(ni == me)
            def _(d=d):
                edge_part(d == 0).wait_recv()
                for q in range(RS_PIECES):
                    rs = pl.ds(q * piece, piece)
                    add_squares(part[d, rs].astype(F32) + cots[rs].astype(F32))

    def originate(d):
        if d > 0:

            @pl.when(ni == 0)
            def _():
                sum_send(0, d, True)

        if d < last:

            @pl.when(ni == last)
            def _():
                sum_send(last, d, False)

    right_side = sbuf.at[...]

    def expert_chunk(c):
        product = dot_rows(hbuf[c][...], right_side[...].reshape(-1, s_width))
        egrads[c][...] = product
        add_squares(product)

    todo = list(dest_order)
    for k in range(1, n_narrow):
        for c in range(chunks):
            hidden_step(k, c)
            if k == 1 and c >= 3 and (c - 3) % 2 == 0 and len(todo) > 2:
                d = todo.pop(0)
                make_part(d)
                originate(d)
            if k == 2 and c == 1:
                while todo:
                    make_part(todo.pop(0))
                for d in dest_order[2:]:
                    if d > 0:

                        @pl.when(ni == 0)
                        def _(d=d):
                            sum_send(0, d, True)

                for d in dest_order[:1:-1]:
                    if d < last:

                        @pl.when(ni == last)
                        def _(d=d):
                            sum_send(last, d, False)

                grant_spare()
                vgrad[...] = part[ni].astype(F32)
            if k == 2 and c == 3:
                send_edge_part()
                for j in range(1, n_narrow):
                    r = lax.rem(ni + n_narrow - j, n_narrow)
                    slot_arrival(r, wi).wait_recv()
                    for m in range(1, n_wide):
                        slot_relay(r, m).start()
            if k == 2 and c == chunks - 1:
                sum_slot(0)
                for copy in own_hidden:
                    copy.wait()
                for j in range(n_narrow):
                    for m in range(1, n_wide):
                        slot_arrival(j, lax.rem(wi + m, n_wide)).wait_recv()
            if k == 3:
                expert_chunk(c)
                if c % 2 == 1:
                    sum_slot(1 + c // 2)
    edge_squares()

    def sum_out(p):
        peer = lax.rem((si * n_wide + wi) * n_narrow + ni + p, n_devices)
        device = (
            lax.div(peer, n_wide * n_narrow),
            lax.rem(lax.div(peer, n_narrow), n_wide),
            lax.rem(peer, n_narrow),
        )
        return remote(own_sum, sums.at[p], g_send.at[0], g_recv.at[0], device)

    def all_sums():
        others = sums.at[pl.ds(1, n_devices - 1)]
        return remote(others, others, g_send.at[0], g_recv.at[0], right)

    own_sum[...] = jnp.sum(mine[...], axis=0, keepdims=True)
    sums[0] = own_sum[...]
    lax.fori_loop(1, n_devices, lambda p, _: [sum_out(p).start()] and 0, 0)
    for me, d in ((1, 0), (last - 1, last)):

        @pl.when(ni == me)
        def _(d=d):
            sum_copy(d, RS_PIECES - 1, d == last, d == last).start()

    for i in range(n_narrow):

        @pl.when(ni == i)
        def _(i=i):
            for c in range(chunks):
                for rightward in (True, False):
                    n_sent = i + 1 if rightward else n_narrow - i
                    if i == (last if rightward else 0):
                        continue
                    sent = hbuf[c].at[pl.ds(0, n_sent * h_rows)]
                    sem = (h_right if rightward else h_left).at[c]
                    remote(sent, sent, sem, h_recv.at[0, c], right).wait_send()

    for copy in own_weights:
        copy.start()

    for edge in (0, last):

        @pl.when(ni == edge)
        def _(edge=edge):
            edge_part(edge == 0).wait_send()

    for k in range(1, n_wide):
        wide_vc(k, wi).wait_send()
        for d in range(n_narrow):
            wide_rows(k, d, wi).wait_send()
        for r in range(n_narrow):
            slot_relay(r, k).wait_send()
    for k in range(1, n_narrow):
        slot_copy(k).wait_send()
    for d in range(n_narrow):

        @pl.when(ni < d)
        def _(d=d):
            remote(part.at[d], rbuf.at[d], r_right.at[d], r_last.at[0], right).wait_send()

        @pl.when(ni > d)
        def _(d=d):
            remote(part.at[d], rbuf.at[d], r_left.at[d], r_last.at[0], left).wait_send()

    for copy in own_moment:
        copy.wait()
    for copy in own_weights:
        copy.wait()
    all_sums().wait_send()
    sum_slot(2 * (last - 1))
    all_sums().wait_recv()
    total[...] = jnp.zeros_like(total) + jnp.sum(sums[...])


def update_kernel(entries, chunks, split, slots, total, vgrad, *refs):
    egrads, emoms, refs = refs[:chunks], refs[chunks : 2 * chunks], refs[2 * chunks :]
    run_update(entries, split, slots, total, vgrad, egrads, emoms, refs[:chunks], *refs[chunks:])


def run_update(
    entries,
    split,
    slots,
    total,
    vgrad,
    egrads,
    emoms,
    weights,
    vm_ref,
    vw_ref,
    ew_out,
    em_out,
    vw_out,
    vm_out,
    vmom,
    vweights,
    em_stage,
    ew_stage,
    vm_stage,
    vw_stage,
    out_sem,
    v_sem,
):
    tile = egrads[0].shape[0] // split
    tiles = len(egrads) * split

    c_width = weights[0].shape[1]

    def out(t):
        rs = pl.ds(t * tile, tile)
        slot = t % slots
        return (
            pltpu.make_async_copy(em_stage.at[slot], em_out.at[rs], out_sem.at[slot, 0]),
            pltpu.make_async_copy(ew_stage.at[slot], ew_out.at[rs], out_sem.at[slot, 1]),
        )

    v_in = (
        pltpu.make_async_copy(vm_ref, vmom, v_sem.at[0]),
        pltpu.make_async_copy(vw_ref, vweights, v_sem.at[1]),
    )
    v_out = (
        pltpu.make_async_copy(vm_stage, vm_out, v_sem.at[2]),
        pltpu.make_async_copy(vw_stage, vw_out, v_sem.at[3]),
    )
    for copy in v_in:
        copy.start()
    factor = jnp.minimum(1.0, math.sqrt(entries) / jnp.sqrt(total[0:1, 0:1] + 1e-06))
    for t in range(tiles):
        slot = t % slots
        if t >= slots:
            for copy in out(t - slots):
                copy.wait()
        c, row = t // split, t % split * tile
        inner = pl.ds(row, tile)
        for j in range(em_stage.shape[2] // c_width):
            cols = pl.ds(j * c_width, c_width)
            moment = MOMENTUM_DECAY * emoms[c][inner, cols] + factor * egrads[c][inner, cols]
            weight = weights[c][pl.ds(j * c_width + row, tile)]
            em_stage[slot, :, cols] = moment
            ew_stage[slot, :, cols] = (weight.astype(F32) - STEP_RATE * moment).astype(BF16)
        for copy in out(t):
            copy.start()
    for copy in v_in:
        copy.wait()
    moment = MOMENTUM_DECAY * vmom[...] + factor * vgrad[...]
    vm_stage[...] = moment
    vw_stage[...] = (vweights[...].astype(F32) - STEP_RATE * moment).astype(BF16)
    for copy in v_out:
        copy.start()
    for t in range(max(tiles - slots, 0), tiles):
        for copy in out(t):
            copy.wait()
    for copy in v_out:
        copy.wait()


def on_device(
    normed_inputs,
    value_cotangent,
    expert_hidden,
    expert_cotangent,
    slot_gate,
    slot_count,
    expert_weight,
    expert_moment,
    value_weight,
    value_moment,
):
    n_section = lax.axis_size("section")
    n_wide = lax.axis_size("wide")
    n_narrow = lax.axis_size("narrow")
    width, kv = normed_inputs.shape[-1], value_cotangent.shape[-1]
    x = normed_inputs.reshape(-1, width)
    vc = value_cotangent.reshape(-1, kv)
    hidden = expert_hidden.reshape(-1, expert_hidden.shape[-1])
    cotangent = expert_cotangent[0, 0]
    micro, slots, _ = cotangent.shape
    in_hbm = functools.partial(pltpu.with_memory_space_constraint, memory_space=pltpu.HBM)
    tokens = x.shape[0]
    h_rows, ff = hidden.shape
    chunks = column_chunks(ff)
    r_width = width // (n_wide * n_narrow)
    s_width = width // n_narrow
    piece = RS_PIECES
    n_devices = n_section * n_wide * n_narrow
    dma = pltpu.SemaphoreType.DMA
    hbm = pl.BlockSpec(memory_space=pltpu.HBM)
    vmem = pl.BlockSpec(memory_space=pltpu.VMEM)
    block = pltpu.VMEM((ff // chunks, s_width), F32)
    w_block = pltpu.VMEM((n_narrow * h_rows, ff // chunks), BF16)
    scratch = [
        pltpu.VMEM((n_narrow, micro, n_wide, slots, s_width), BF16),
        pltpu.VMEM((micro, slots, width), BF16),
        pltpu.VMEM((n_narrow, n_wide * tokens, r_width), BF16),
        pltpu.VMEM((n_wide * tokens, kv), BF16),
        pltpu.VMEM((n_narrow, r_width, kv), BF16),
        pltpu.VMEM((n_narrow, r_width, kv), BF16),
        pltpu.VMEM((r_width, kv), BF16),
        pltpu.VMEM((n_devices, 1, 128), F32),
        pltpu.VMEM((1, 128), F32),
        pltpu.VMEM((8, 128), F32),
    ]
    *blocks, vgrad, total = pl.pallas_call(
        functools.partial(gather_kernel, (n_section, n_wide, n_narrow, chunks)),
        out_shape=(
            *[block] * (2 * chunks),
            *[w_block] * chunks,
            pltpu.VMEM((r_width, kv), F32),
            pltpu.VMEM((8, 128), F32),
        ),
        in_specs=[hbm, hbm, hbm, hbm, vmem, vmem, hbm, hbm],
        out_specs=(vmem,) * (3 * chunks + 2),
        scratch_shapes=[
            *scratch,
            dma((n_narrow, chunks)),
            dma((chunks,)),
            dma((chunks,)),
            dma((n_narrow, n_wide)),
            dma((n_narrow,)),
            dma((n_narrow, n_wide)),
            dma((n_wide, n_narrow + 1)),
            dma((n_wide, n_narrow + 1)),
            dma((n_narrow, piece)),
            dma((piece,)),
            dma((n_narrow,)),
            dma((n_narrow,)),
            dma((1,)),
            dma((1,)),
            dma((2 + n_narrow + (2 + s_width * chunks // ff) * chunks,)),
            dma((1,)),
            dma((1,)),
            pltpu.SemaphoreType.REGULAR,
        ],
        compiler_params=pltpu.CompilerParams(
            collective_id=0, has_side_effects=True, vmem_limit_bytes=grant(scratch)
        ),
    )(
        *(in_hbm(a) for a in (x, vc, hidden, cotangent)),
        slot_gate[0, 0],
        slot_count[0],
        in_hbm(expert_moment[0]),
        in_hbm(expert_weight[0]),
    )

    total, vgrad, *blocks = (
        pltpu.with_memory_space_constraint(a, pltpu.VMEM) for a in (total, vgrad, *blocks)
    )
    layer_entries = ff * s_width + r_width * kv
    entries = n_section * n_wide * n_narrow * layer_entries
    split, depth = 2, 6
    tiles = chunks * split
    tile = ff // tiles
    update_scratch = [
        pltpu.VMEM((r_width, kv), F32),
        pltpu.VMEM((r_width, kv), BF16),
        pltpu.VMEM((depth, tile, s_width), F32),
        pltpu.VMEM((depth, tile, s_width), BF16),
        pltpu.VMEM((r_width, kv), F32),
        pltpu.VMEM((r_width, kv), BF16),
    ]
    outs = pl.pallas_call(
        functools.partial(update_kernel, entries, chunks, split, depth),
        out_shape=(
            jax.ShapeDtypeStruct((ff, s_width), BF16),
            jax.ShapeDtypeStruct((ff, s_width), F32),
            jax.ShapeDtypeStruct((r_width, kv), BF16),
            jax.ShapeDtypeStruct((r_width, kv), F32),
        ),
        in_specs=[vmem] * (3 * chunks + 2) + [hbm] * 2,
        out_specs=(hbm, hbm, hbm, hbm),
        scratch_shapes=[
            *update_scratch,
            dma((depth, 2)),
            dma((4,)),
        ],
        compiler_params=pltpu.CompilerParams(vmem_limit_bytes=grant(update_scratch)),
    )(total, vgrad, *blocks, *(in_hbm(a[0]) for a in (value_moment, value_weight)))
    return tuple(o[None] for o in outs)


def solution(mesh):
    return jax.shard_map(
        on_device,
        mesh=mesh,
        in_specs=(
            P("section", "narrow", None, "wide", None),
            P("section", "narrow", None, "wide", None),
            P("section", "narrow", None, None, "wide"),
            P("section", "narrow", None, "wide", None),
            P("section", "narrow", None, "wide"),
            P("section", "narrow", None),
            P("section", "wide", "narrow"),
            P("section", "wide", "narrow"),
            P("section", ("wide", "narrow"), None),
            P("section", ("wide", "narrow"), None),
        ),
        out_specs=(
            P("section", "wide", "narrow"),
            P("section", "wide", "narrow"),
            P("section", ("wide", "narrow"), None),
            P("section", ("wide", "narrow"), None),
        ),
        check_vma=False,
    )
```
